32 devices in a mesh: samp: 16 (over z, y, x), tgt: 2 (over core).
Axes of the slice: x: 2, y: 2, z: 4, core: 2. Of those that a mesh axis runs over, the one named last changes fastest.
Arguments:
- samples: bfloat16 [3072, 128], P('samp'), may hold values from -6 to 6
- omega: bfloat16 [128, 4096], replicated, may hold values from -0.5 to 0.5
- phase: float32 [4096], replicated, may hold values from -3.140625 to 3.140625
- right_side: float32 [4096, 512], P('samp', 'tgt'), may hold values from -6 to 6
Outputs:
- weights: float32 [4096, 512], P('samp', 'tgt')
The draws below stay inside these ranges and needn't reach their ends.
All inputs are finite; a program needn't handle non-finite values.
Results may differ from the reference program's by a relative error of at most 0.011.
The reference program's roundings to bfloat16 on the way count: a program that leaves them out, or rounds other values in their place, can miss the bound.
Values may be sent and summed in bfloat16 or wider, within the bound.
A program may use at most 128 MiB of HBM per device.

```python
import jax
import jax.numpy as jnp
from jax import lax

F = 4096
K = 512
DX = 128
ITERS = 2
N = 3072


def steps_of(rng, shape, shards, least, top_value):
    factor_of = 1.0
    for dim, blocks in shards:
        heights = jax.random.uniform(jax.random.fold_in(jax.random.fold_in(rng, 6), dim), (blocks,), jnp.float32, least / len(shards), top_value / len(shards))
        factor_of = factor_of * jnp.repeat(jnp.exp(heights), shape[dim] // blocks).reshape((-1,) + (1,) * (len(shape) - 1 - dim))
    return factor_of


def gaussian(rng, shape, deviation, bound, shards=(), held_as=jnp.bfloat16):
    values = jax.random.normal(rng, shape, jnp.float32) * deviation
    if len(shards) > 0:
        values = steps_of(rng, shape, shards, -0.22, 0.18) * values
    return jnp.clip(values, min=-bound, max=bound).astype(held_as)


def setup_inputs(seed: int = 0) -> dict:
    streams_of = jax.random.split(jax.random.key(seed), 5)
    return {
        "samples": gaussian(streams_of[0], (N, DX), 1.0, 6.0, ((0, 16),)),
        "omega": gaussian(streams_of[1], (DX, F), DX ** -0.5, 0.5),
        "phase": jnp.clip(jax.random.uniform(streams_of[2], (F,), jnp.float32, -3.140625, 3.140625), -3.140625, 3.140625),
        "right_side": gaussian(streams_of[3], (F, K), 1.0, 6.0, ((0, 16), (1, 2)), jnp.float32),
    }


ridge = 1.0

def precise_dot(left_matrix, right_matrix):
    return jnp.dot(left_matrix, right_matrix, precision=lax.Precision.HIGHEST)

def spd_solve(gram_matrix, rhs_matrix):
    factor = jnp.linalg.cholesky(gram_matrix)
    return jax.scipy.linalg.cho_solve((factor, True), rhs_matrix)

def reference(samples, omega, phase, right_side):
    preact = jnp.dot(samples.astype(jnp.float32), omega.astype(jnp.float32), preferred_element_type=jnp.float32) + phase
    features = jnp.cos(preact).astype(jnp.bfloat16)
    sample_total = features.shape[0]
    weights = jnp.zeros_like(right_side)
    residual = right_side
    direction = right_side
    gram_rr = precise_dot(residual.T, residual)
    for iteration in range(ITERS):
        projected = jnp.dot(features.astype(jnp.float32), direction.astype(jnp.bfloat16).astype(jnp.float32), preferred_element_type=jnp.float32).astype(jnp.bfloat16)
        image = jnp.dot(features.T.astype(jnp.float32), projected.astype(jnp.float32), preferred_element_type=jnp.float32) / sample_total + ridge * direction
        alpha_coef = spd_solve(precise_dot(direction.T, image), gram_rr)
        weights = weights + precise_dot(direction, alpha_coef)
        residual = residual - precise_dot(image, alpha_coef)
        gram_new = precise_dot(residual.T, residual)
        beta_coef = spd_solve(gram_rr, gram_new)
        direction = residual + precise_dot(direction, beta_coef)
        gram_rr = gram_new
    return weights
```

```python
import functools

import jax
import jax.numpy as jnp
from jax import lax
from jax.experimental import pallas as pl
from jax.experimental.pallas import tpu as pltpu
from jax.sharding import PartitionSpec as P

ridge = 1.0
HI = lax.Precision.HIGHEST
F32 = jnp.float32
BF16 = jnp.bfloat16
BLOCK = 128
GROUP = 8
PLANE = 4
MESH = pl.DeviceIdType.MESH
NN = (((1,), (0,)), ((), ()))
TN = (((0,), (0,)), ((), ()))
NT = (((1,), (1,)), ((), ()))
VMEM = pl.BlockSpec(memory_space=pltpu.VMEM)


def precise_dot(left_matrix, right_matrix):
    return jnp.dot(left_matrix, right_matrix, precision=HI, preferred_element_type=F32)


def dot(left, right, dims=NN):
    return lax.dot_general(left, right, dims, preferred_element_type=F32)


def halves(x):
    high = x.astype(BF16)
    return high, (x - high.astype(F32)).astype(BF16)


def dot_halves(left, right, dims=NN):
    return dot(left[0], right[0], dims) + (dot(left[0], right[1], dims) + dot(left[1], right[0], dims))


def cosine(x):
    turns = x * 0.15915494309189535
    f = turns - jnp.round(turns)
    s = f * f
    p = -21.071105627575776
    for coef in (
        58.790492120100176,
        -85.27162153429538,
        64.92865742103322,
        -19.738980355764014,
        0.999999210782322,
    ):
        p = p * s + coef
    return p


def sweep(held):
    size = len(held)
    at = lambda i, j: held[max(i, j)][min(i, j)]
    for p in range(size):
        inverse = 1.0 / held[p][p]
        column = [at(i, p) for i in range(size)]
        scaled = [c * inverse for c in column]
        for i in range(size):
            for j in range(i + 1):
                if i == p and j == p:
                    held[i][j] = -inverse
                elif i == p:
                    held[i][j] = scaled[j]
                elif j == p:
                    held[i][j] = scaled[i]
                else:
                    held[i][j] = held[i][j] - scaled[i] * column[j]
    return [[-at(i, j) for j in range(size)] for i in range(size)]


def invert_block(value):
    size = value.shape[0]
    tiles = [value[t * 8 : t * 8 + 8, :] for t in range(size // 8)]
    lane = lax.broadcasted_iota(jnp.int32, (8, size), 1)
    sub = lax.broadcasted_iota(jnp.int32, (8, size), 0)
    for g in range(size // GROUP):
        j = g * GROUP
        in_group = (lane >= j) & (lane < j + GROUP)
        home = tiles[g]
        spread = [jnp.broadcast_to(home[:, j + m : j + m + 1], (8, size)) for m in range(GROUP)]
        rows = [jnp.broadcast_to(home[k : k + 1, :], (8, size)) for k in range(GROUP)]
        pivots = sweep(
            [[jnp.broadcast_to(spread[m][k : k + 1, :], (8, size)) for m in range(k + 1)] for k in range(GROUP)]
        )
        scaled = []
        for k in range(GROUP):
            terms = [pivots[k][m] * rows[m] for m in range(GROUP)]
            while len(terms) > 1:
                terms = [terms[i] + terms[i + 1] for i in range(0, len(terms), 2)]
            line = terms[0]
            for m in range(GROUP):
                line = jnp.where(lane == j + m, pivots[k][m], line)
            scaled.append(line)
        nxt = []
        for t, tile in enumerate(tiles):
            if t == g:
                new = scaled[0]
                for k in range(1, GROUP):
                    new = jnp.where(sub == k, scaled[k], new)
            else:
                terms = [jnp.broadcast_to(tile[:, j + k : j + k + 1], (8, size)) * scaled[k] for k in range(GROUP)]
                while len(terms) > 1:
                    terms = [terms[i] + terms[i + 1] for i in range(0, len(terms), 2)]
                new = jnp.where(in_group, 0.0, tile) - terms[0]
            nxt.append(new)
        tiles = nxt
    return jnp.concatenate(tiles, axis=0)


def inverse_kernel(gram_ref, work):
    total = gram_ref.shape[0]
    size = BLOCK
    work[...] = gram_ref[...]

    def step(k, carry):
        at = pl.ds(pl.multiple_of(k * size, size), size)
        inv = invert_block(work[at, at])
        work[at, :] = precise_dot(inv, work[at, :])
        work[at, at] = inv
        row = work[at, :]
        for i in range(total // size):
            rows = pl.ds(i * size, size)
            block = work[rows, at]
            work[rows, at] = jnp.where(k == i, block, 0.0)
            work[rows, :] = work[rows, :] - precise_dot(jnp.where(k == i, 0.0, block), row)
        return carry

    lax.fori_loop(0, total // size, step, 0)


def inverse_of(gram):
    total = gram.shape[0]
    return pl.pallas_call(
        inverse_kernel,
        out_shape=jax.ShapeDtypeStruct((total, total), F32),
        in_specs=[VMEM],
        out_specs=VMEM,
        compiler_params=pltpu.CompilerParams(vmem_limit_bytes=16 * 2**20),
        cost_estimate=pl.CostEstimate(flops=2 * 10**10, bytes_accessed=2 * 2**20, transcendentals=0),
        name="inverse",
    )(gram)


def last_kernel(gram_ref, rhs_ref, right_ref, first_ref, direction_ref, out_ref, work, side):
    total = gram_ref.shape[0]
    size = BLOCK
    work[...] = gram_ref[...]
    side[...] = rhs_ref[...]

    def step(k, carry):
        at = pl.ds(pl.multiple_of(k * size, size), size)
        inv = invert_block(work[at, at])
        row_a = precise_dot(inv, work[at, :])
        row_x = precise_dot(inv, side[at, :])
        for i in range(total // size):
            rows = pl.ds(i * size, size)
            left = jnp.where(k == i, 0.0, work[rows, at])
            work[rows, :] = work[rows, :] - precise_dot(left, row_a)
            side[rows, :] = side[rows, :] - precise_dot(left, row_x)
        work[at, :] = row_a
        side[at, :] = row_x
        return carry

    lax.fori_loop(0, total // size, step, 0)
    out_ref[...] = dot_halves(halves(right_ref[...]), halves(first_ref[...])) + dot_halves(
        halves(direction_ref[...]), halves(side[...])
    )


def last_solve(gram, rhs, right_all, first, direction):
    total, cols = rhs.shape
    return pl.pallas_call(
        last_kernel,
        out_shape=jax.ShapeDtypeStruct((direction.shape[0], cols), F32),
        in_specs=[VMEM] * 5,
        out_specs=VMEM,
        scratch_shapes=[pltpu.VMEM((total, total), F32), pltpu.VMEM((total, cols), F32)],
        compiler_params=pltpu.CompilerParams(vmem_limit_bytes=24 * 2**20),
        cost_estimate=pl.CostEstimate(flops=2 * 10**10, bytes_accessed=3 * 2**20, transcendentals=0),
        name="last",
    )(gram, rhs, right_all, first, direction)


class Place:
    def __init__(self, n, groups):
        self.n, self.groups, self.lines = n, groups, n // PLANE
        self.me, self.col = lax.axis_index("samp"), lax.axis_index("tgt")
        self.inner = lax.rem(self.me, PLANE)
        self.line = lax.div(self.me, PLANE)
        self.over_x = self.me + 1 - 2 * lax.rem(self.me, 2)
        self.over_y = self.me + 2 - 4 * lax.div(self.inner, 2)
        self.inner_x = lax.rem(self.over_x, PLANE)
        self.inner_y = lax.rem(self.over_y, PLANE)
        self.along = [lax.rem(self.line + s, self.lines) * PLANE + self.inner for s in range(1, self.lines)]
        self.others = [lax.rem(self.col + s, groups) for s in range(1, groups)]

    def meet(self):
        barrier = pltpu.get_barrier_semaphore()
        for peer in [*self.along, self.over_x, self.over_y]:
            pl.semaphore_signal(barrier, inc=1, device_id={"samp": peer}, device_id_type=MESH)
        for other in self.others:
            pl.semaphore_signal(barrier, inc=1, device_id={"tgt": other}, device_id_type=MESH)
        pl.semaphore_wait(barrier, len(self.along) + 2 + len(self.others))

    def behind(self, s, inner):
        return lax.rem(self.line + self.lines - s, self.lines) * PLANE + inner


class Gather:
    def __init__(self, place, slab, rows, sends, recvs):
        self.place, self.slab, self.rows, self.sends, self.recvs = place, slab, rows, sends, recvs
        self.started = []
        self.z, self.x, self.y, self.d = {}, {}, {}, []

    def span(self, block, part=None):
        if part is None:
            return self.slab.at[pl.ds(pl.multiple_of(block * self.rows, self.rows), self.rows)]
        half = self.rows // 2
        return self.slab.at[pl.ds(pl.multiple_of(block * self.rows + part * half, half), half)]

    def send(self, ref, slot, peer):
        copy = pltpu.make_async_remote_copy(
            src_ref=ref,
            dst_ref=ref,
            send_sem=self.sends.at[slot],
            recv_sem=self.recvs.at[slot],
            device_id={"samp": peer},
            device_id_type=MESH,
        )
        copy.start()
        self.started.append(copy)
        return copy

    def across(self, s):
        p = self.place
        ref = self.span(p.behind(s, p.inner))
        base = p.lines + 4 * s
        self.x[s] = self.send(ref, base, p.over_x)
        self.y[s] = self.send(ref, base + 1, p.over_y)

    def open(self):
        p = self.place
        for s in range(1, p.lines):
            self.z[s] = self.send(self.span(p.me), s, p.along[s - 1])
        self.across(0)

    def relay(self, s):
        self.z[s].wait_recv()
        self.across(s)

    def corner(self, s):
        p = self.place
        base = p.lines + 4 * s
        self.x[s].wait_recv()
        self.d.append(self.send(self.span(p.behind(s, p.inner_x), 0), base + 2, p.over_y))
        self.y[s].wait_recv()
        self.d.append(self.send(self.span(p.behind(s, p.inner_y), 1), base + 3, p.over_x))

    def actions(self):
        steps = []
        for s in range(1, self.place.lines):
            steps.append(functools.partial(self.relay, s))
            steps.append(functools.partial(self.corner, s - 1))
        steps.append(functools.partial(self.corner, self.place.lines - 1))
        return steps

    def close(self):
        for copy in self.d:
            copy.wait_recv()

    def drain(self):
        for copy in self.started:
            copy.wait_send()


def room(groups):
    return (63 if groups > 2 else 40) * 2**20


def slots(n):
    return n // PLANE + 4 * (n // PLANE)


class Swap:
    def __init__(self, place, src, dst, sends, recvs, base, slotted=False):
        self.copies = []
        for i, other in enumerate(place.others):
            copy = pltpu.make_async_remote_copy(
                src_ref=src,
                dst_ref=dst.at[i] if slotted else dst,
                send_sem=sends.at[base + i],
                recv_sem=recvs.at[base + i],
                device_id={"tgt": other},
                device_id_type=MESH,
            )
            copy.start()
            self.copies.append(copy)

    def wait(self):
        for copy in self.copies:
            copy.wait_recv()

    def drain(self):
        for copy in self.copies:
            copy.wait_send()


def interleave(actions, work):
    done = 0
    for i, piece in enumerate(work):
        upto = (i + 1) * len(actions) // len(work)
        piece()
        for act in actions[done:upto]:
            act()
        done = upto


def beside(parts):
    return parts[0] if len(parts) == 1 else jnp.concatenate(parts, axis=1)


def first_kernel(
    n, groups, total_n,
    samples_ref, omega_ref, phase_ref, right_ref,
    gram_ref, mixed_ref, lifted_ref, part_ref, proj_ref, feats_ref,
    spots, flat, rights, projs, lifts, g_sends, g_recvs, s_sends, s_recvs,
):
    place = Place(n, groups)
    me, col = place.me, place.col
    rows, depth = samples_ref.shape
    feats, cols = right_ref.shape
    total_f = omega_ref.shape[1]
    mine = total_f // groups
    targets = groups * cols
    pieces, piece = spots.shape[0], spots.shape[1] // n
    slab = col if pieces > 1 else 0

    spots[slab, pl.ds(pl.multiple_of(me * piece, piece), piece), :] = samples_ref[
        pl.ds(pl.multiple_of(slab * piece, piece), piece), :
    ]
    rights[col, pl.ds(pl.multiple_of(me * feats, feats), feats), :] = right_ref[...].astype(BF16)
    place.meet()
    near = Gather(place, spots.at[slab], piece, g_sends.at[0], g_recvs.at[0])
    far = Gather(place, rights.at[col], feats, g_sends.at[1], g_recvs.at[1])
    near.open()
    far.open()

    tile = 256
    quarter = total_f // 4

    def own_features(part):
        def one(i, carry):
            at = pl.ds(pl.multiple_of(part * quarter + i * tile, tile), tile)
            feats_ref[:, at] = cosine(dot(samples_ref[...], omega_ref[:, at]) + phase_ref[:, at]).astype(BF16)
            return carry

        lax.fori_loop(0, quarter // tile, one, 0)

    interleave(near.actions(), [functools.partial(own_features, part) for part in range(4)])
    near.close()
    swaps = []
    if pieces > 1:
        swap = Swap(place, spots.at[col], spots.at[col], s_sends, s_recvs, 0)
        swaps.append(swap)
        swap.wait()

    def settle(b, carry):
        for t in range(pieces):
            flat[pl.ds(pl.multiple_of(b * rows + t * piece, piece), piece), :] = spots[
                t, pl.ds(pl.multiple_of(b * piece, piece), piece), :
            ]
        return carry

    lax.fori_loop(0, n, settle, 0)

    splits = 2
    tiles = total_n // tile // splits

    def lift_features(c, part):
        at = pl.ds(pl.multiple_of(col * mine + c * tile, tile), tile)
        weights = omega_ref[:, at].T
        shift = jnp.broadcast_to(phase_ref[:, at], (128, tile)).T
        shift = jnp.concatenate([shift] * (tile // 128), axis=1)
        down = pl.ds(c * tile, tile)

        def one(i, carry):
            over = pl.ds(pl.multiple_of((part * tiles + i) * tile, tile), tile)
            lifts[down, over] = cosine(dot(weights, flat[over, :], NT) + shift).astype(BF16)
            return carry

        lax.fori_loop(0, tiles, one, 0)

    interleave(
        far.actions(),
        [functools.partial(lift_features, c, part) for c in range(mine // tile) for part in range(splits)],
    )
    far.close()
    spread = Swap(place, rights.at[col], rights.at[col], s_sends, s_recvs, groups)
    swaps.append(spread)
    projs[col, pl.ds(pl.multiple_of(me * rows, rows), rows), :] = dot(feats_ref[...], rights[col]).astype(BF16)
    last = Gather(place, projs.at[col], rows, g_sends.at[2], g_recvs.at[2])
    last.open()

    chunk = 512
    spread.wait()

    def gram_piece(lo, hi):
        def one(i, carry):
            at = pl.ds(pl.multiple_of(i * chunk, chunk), chunk)
            block = beside([rights[t, at, :] for t in range(groups)])
            gram_ref[...] += dot(block, block, TN)
            return carry

        lax.fori_loop(lo, hi, one, 0)

    gram_ref[...] = jnp.zeros_like(gram_ref)
    count = total_f // chunk
    interleave(last.actions(), [functools.partial(gram_piece, i * count // 4, (i + 1) * count // 4) for i in range(4)])
    last.close()
    swap = Swap(place, projs.at[col], projs.at[col], s_sends, s_recvs, 2 * groups)
    swaps.append(swap)

    def lift(which):
        def one(i, carry):
            at = pl.ds(pl.multiple_of(i * chunk, chunk), chunk)
            lifted_ref[which, at, :] = dot(lifts[at, :], projs[which]) * (1.0 / total_n)
            return carry

        lax.fori_loop(0, mine // chunk, one, 0)

    lift(col)
    swap.wait()
    for other in place.others:
        lift(other)

    mixed_ref[...] = jnp.zeros_like(mixed_ref)

    def mix(i, carry):
        at = pl.ds(pl.multiple_of(i * chunk, chunk), chunk)
        block = beside([projs[t, at, :] for t in range(groups)])
        mixed_ref[...] += dot(block, block, TN)
        return carry

    lax.fori_loop(0, total_n // chunk, mix, 0)
    mixed_ref[...] = mixed_ref[...] * (1.0 / total_n) + ridge * gram_ref[...]
    own = pl.ds(pl.multiple_of(me * rows, rows), rows)
    for t in range(groups):
        part_ref[t] = rights[t, pl.ds(pl.multiple_of(col * mine, mine), mine), :]
        proj_ref[:, t * cols : (t + 1) * cols] = projs[t, own, :]
    for gather in (near, far, last):
        gather.drain()
    for swap in swaps:
        swap.drain()


def first_stage(samples, omega, phase, right_side):
    n, groups = lax.axis_size("samp"), lax.axis_size("tgt")
    rows, depth = samples.shape
    feats, cols = right_side.shape
    total_f = omega.shape[1]
    total_n, mine, targets = rows * n, total_f // groups, cols * groups
    pieces = groups if rows % (32 * groups) == 0 else 1
    return pl.pallas_call(
        functools.partial(first_kernel, n, groups, total_n),
        out_shape=[
            jax.ShapeDtypeStruct((targets, targets), F32),
            jax.ShapeDtypeStruct((targets, targets), F32),
            jax.ShapeDtypeStruct((groups, mine, cols), F32),
            jax.ShapeDtypeStruct((groups, mine, cols), BF16),
            jax.ShapeDtypeStruct((rows, targets), BF16),
            jax.ShapeDtypeStruct((rows, total_f), BF16),
        ],
        in_specs=[VMEM] * 4,
        out_specs=[VMEM] * 6,
        scratch_shapes=[
            pltpu.VMEM((pieces, total_n // pieces, depth), BF16),
            pltpu.VMEM((total_n, depth), BF16),
            pltpu.VMEM((groups, total_f, cols), BF16),
            pltpu.VMEM((groups, total_n, cols), BF16),
            pltpu.VMEM((mine, total_n), BF16),
            pltpu.SemaphoreType.DMA((3, slots(n))),
            pltpu.SemaphoreType.DMA((3, slots(n))),
            pltpu.SemaphoreType.DMA((3 * groups,)),
            pltpu.SemaphoreType.DMA((3 * groups,)),
        ],
        compiler_params=pltpu.CompilerParams(collective_id=0, has_side_effects=True, vmem_limit_bytes=room(groups)),
        cost_estimate=pl.CostEstimate(flops=10**11, bytes_accessed=2 * 2**20, transcendentals=0),
        name="first",
    )(samples, omega, phase.reshape(1, -1), right_side)


def second_kernel(
    n, groups, total_n,
    inverse_ref, gram_ref, lifted_ref, part_ref, proj_ref, feats_ref,
    first_ref, target_ref, final_ref, direction_ref,
    resid, sums, theirs, aside, away, projs, shared, g_sends, g_recvs, s_sends, s_recvs,
):
    place = Place(n, groups)
    me, col = place.me, place.col
    rows = feats_ref.shape[0]
    mine, cols = lifted_ref.shape[1:]
    targets = groups * cols
    chunk = 512
    place.meet()
    inverse = halves(inverse_ref[...])
    alpha = dot_halves(inverse, halves(gram_ref[...]))
    alpha_halves = halves(alpha)
    for t in range(groups):
        pl.when(col == t)(functools.partial(first_ref.__setitem__, Ellipsis, alpha[:, t * cols : (t + 1) * cols]))
    sums[...] = jnp.zeros_like(sums)
    aside[...] = jnp.zeros_like(aside)

    def one(i, carry):
        at = pl.ds(pl.multiple_of(i * chunk, chunk), chunk)
        right = beside([part_ref[t, at, :] for t in range(groups)]).astype(F32)
        image = halves(beside([lifted_ref[t, at, :] for t in range(groups)]) + ridge * right)
        left = right - dot_halves(image, alpha_halves)
        resid[at, :] = left
        pair = halves(left)
        sums[0] += dot_halves(image, pair, TN)
        sums[1] += dot_halves(pair, pair, TN)
        over = pl.ds(pl.multiple_of(col * mine + i * chunk, chunk), chunk)
        aside[...] += dot(feats_ref[:, over], pair[0])
        return carry

    lax.fori_loop(0, mine // chunk, one, 0)
    swaps = [
        Swap(place, sums.at[0], theirs.at[0], s_sends, s_recvs, 0, True),
        Swap(place, aside, away, s_sends, s_recvs, groups, True),
        Swap(place, sums.at[1], theirs.at[1], s_sends, s_recvs, 2 * groups, True),
    ]
    swaps[0].wait()

    def total(which):
        value = sums[which]
        for i in range(groups - 1):
            value = value + theirs[which, i]
        return value

    beta = -dot_halves(inverse, halves(total(0)))
    beta_halves = halves(beta)
    swaps[1].wait()
    value = aside[...]
    for i in range(groups - 1):
        value = value + away[i]
    value = value + dot(proj_ref[...], beta_halves[0]) + dot(proj_ref[...], beta_halves[1])
    own = pl.ds(pl.multiple_of(me * rows, rows), rows)
    for t in range(groups):
        pl.when(col == t)(
            functools.partial(projs.__setitem__, (t, own), value[:, t * cols : (t + 1) * cols].astype(BF16))
        )
    gather = Gather(place, projs.at[col], rows, g_sends, g_recvs)
    gather.open()
    final_ref[...] = jnp.zeros_like(final_ref)

    def turn(i):
        at = pl.ds(i * chunk, chunk)
        right = beside([part_ref[t, at, :] for t in range(groups)])
        line = resid[at, :] + dot(right, beta_halves[0]) + dot(right, beta_halves[1])
        resid[at, :] = line
        pair = halves(line)
        final_ref[...] += dot_halves(pair, pair, TN)

    interleave(gather.actions(), [functools.partial(turn, i) for i in range(mine // chunk)])
    swaps[2].wait()
    swaps.append(Swap(place, final_ref, shared, s_sends, s_recvs, 3 * groups, True))
    feats = direction_ref.shape[0]
    owners = n // groups
    source = lax.div(me, owners)
    held = pl.ds(pl.multiple_of(lax.rem(me, owners) * feats, feats), feats)
    new = total(1)
    for t in range(groups):
        pl.when(col == t)(functools.partial(target_ref.__setitem__, Ellipsis, new[:, t * cols : (t + 1) * cols]))

    def copies():
        return [
            pltpu.make_async_remote_copy(
                src_ref=resid.at[held],
                dst_ref=resid.at[pl.ds(mine, feats)],
                send_sem=s_sends.at[4 * groups + i],
                recv_sem=s_recvs.at[4 * groups],
                device_id={"tgt": other},
                device_id_type=MESH,
            )
            for i, other in enumerate(place.others)
        ]

    @pl.when(col == source)
    def _():
        for copy in copies():
            copy.start()

    gather.close()
    swaps.append(Swap(place, projs.at[col], projs.at[col], s_sends, s_recvs, 5 * groups))
    swaps[3].wait()
    swaps[3].drain()
    value = final_ref[...]
    for i in range(groups - 1):
        value = value + shared[i]
    final_ref[...] = ridge * value
    swaps[4].wait()

    def mix(i, carry):
        at = pl.ds(pl.multiple_of(i * chunk, chunk), chunk)
        block = beside([projs[t, at, :] for t in range(groups)])
        final_ref[...] += dot(block, block, TN) * (1.0 / total_n)
        return carry

    lax.fori_loop(0, total_n // chunk, mix, 0)

    @pl.when(col == source)
    def _():
        direction_ref[...] = resid[held, :]
        for copy in copies():
            copy.wait_send()

    @pl.when(col != source)
    def _():
        copies()[0].wait_recv()
        direction_ref[...] = resid[pl.ds(mine, feats), :]

    gather.drain()
    for swap in swaps[:3] + swaps[4:]:
        swap.drain()


def second_stage(inverse, gram, lifted, part, proj, feats_own, feats):
    n, groups = lax.axis_size("samp"), lax.axis_size("tgt")
    _, mine, cols = lifted.shape
    rows = feats_own.shape[0]
    total_n, targets = rows * n, cols * groups
    return pl.pallas_call(
        functools.partial(second_kernel, n, groups, total_n),
        out_shape=[
            jax.ShapeDtypeStruct((targets, cols), F32),
            jax.ShapeDtypeStruct((targets, cols), F32),
            jax.ShapeDtypeStruct((targets, targets), F32),
            jax.ShapeDtypeStruct((feats, targets), F32),
        ],
        in_specs=[VMEM] * 6,
        out_specs=[VMEM] * 4,
        scratch_shapes=[
            pltpu.VMEM((mine + feats, targets), F32),
            pltpu.VMEM((2, targets, targets), F32),
            pltpu.VMEM((2, max(groups - 1, 1), targets, targets), F32),
            pltpu.VMEM((rows, targets), F32),
            pltpu.VMEM((max(groups - 1, 1), rows, targets), F32),
            pltpu.VMEM((groups, total_n, cols), BF16),
            pltpu.VMEM((max(groups - 1, 1), targets, targets), F32),
            pltpu.SemaphoreType.DMA((slots(n),)),
            pltpu.SemaphoreType.DMA((slots(n),)),
            pltpu.SemaphoreType.DMA((6 * groups,)),
            pltpu.SemaphoreType.DMA((6 * groups,)),
        ],
        compiler_params=pltpu.CompilerParams(collective_id=1, has_side_effects=True, vmem_limit_bytes=room(groups)),
        cost_estimate=pl.CostEstimate(flops=10**11, bytes_accessed=2 * 2**20, transcendentals=0),
        name="second",
    )(inverse, gram, lifted, part, proj, feats_own)


def body(samples, omega, phase, right_side):
    gram, mixed, lifted, part, proj, feats_own = first_stage(samples, omega, phase, right_side)
    inverse = inverse_of(mixed)
    first, target, final, direction = second_stage(
        inverse, gram, lifted, part, proj, feats_own, right_side.shape[0]
    )
    right_all = lax.all_gather(right_side, "tgt", axis=1, tiled=True)
    return last_solve(final, target, right_all, first, direction)


def solution(mesh):
    placed = (P("samp", None), P(), P(), P("samp", "tgt"))
    return jax.shard_map(
        body, mesh=mesh, in_specs=placed, out_specs=P("samp", "tgt"), check_vma=False
    )
```

```python
import functools

import jax
import jax.numpy as jnp
from jax import lax
from jax.experimental import pallas as pl
from jax.experimental.pallas import tpu as pltpu
from jax.sharding import PartitionSpec as P

ridge = 1.0
HI = lax.Precision.HIGHEST
F32 = jnp.float32
BF16 = jnp.bfloat16
BLOCK = 128
GROUP = 8
PLANE = 4
MESH = pl.DeviceIdType.MESH
NN = (((1,), (0,)), ((), ()))
TN = (((0,), (0,)), ((), ()))
NT = (((1,), (1,)), ((), ()))
VMEM = pl.BlockSpec(memory_space=pltpu.VMEM)


def precise_dot(left_matrix, right_matrix):
    return jnp.dot(left_matrix, right_matrix, precision=HI, preferred_element_type=F32)


def dot(left, right, dims=NN):
    return lax.dot_general(left, right, dims, preferred_element_type=F32)


def halves(x):
    high = x.astype(BF16)
    return high, (x - high.astype(F32)).astype(BF16)


def dot_halves(left, right, dims=NN):
    return dot(left[0], right[0], dims) + (dot(left[0], right[1], dims) + dot(left[1], right[0], dims))


def cosine(x):
    turns = x * 0.15915494309189535
    f = turns - jnp.round(turns)
    s = f * f
    p = -21.071105627575776
    for coef in (
        58.790492120100176,
        -85.27162153429538,
        64.92865742103322,
        -19.738980355764014,
        0.999999210782322,
    ):
        p = p * s + coef
    return p


def sweep(held):
    size = len(held)
    at = lambda i, j: held[max(i, j)][min(i, j)]
    for p in range(0, size, 2):
        q = p + 1
        a, b, c = held[p][p], held[q][p], held[q][q]
        scale = 1.0 / (a * c - b * b)
        pp, pq, qq = c * scale, b * scale, a * scale
        first, second = [at(i, p) for i in range(size)], [at(i, q) for i in range(size)]
        rest = [i for i in range(size) if i not in (p, q)]
        left = {i: first[i] * pp - second[i] * pq for i in rest}
        right = {i: second[i] * qq - first[i] * pq for i in rest}
        for i in rest:
            for j in rest:
                if j <= i:
                    held[i][j] = held[i][j] - (left[i] * first[j] + right[i] * second[j])
        for i in rest:
            held[max(i, p)][min(i, p)] = left[i]
            held[max(i, q)][min(i, q)] = right[i]
        held[p][p], held[q][p], held[q][q] = -pp, pq, -qq
    return [[-at(i, j) for j in range(size)] for i in range(size)]


def invert_block(value):
    size = value.shape[0]
    tiles = [value[t * 8 : t * 8 + 8, :] for t in range(size // 8)]
    lane = lax.broadcasted_iota(jnp.int32, (8, size), 1)
    sub = lax.broadcasted_iota(jnp.int32, (8, size), 0)
    for g in range(size // GROUP):
        j = g * GROUP
        in_group = (lane >= j) & (lane < j + GROUP)
        home = tiles[g]
        spread = [jnp.broadcast_to(home[:, j + m : j + m + 1], (8, size)) for m in range(GROUP)]
        rows = [
            jnp.where(in_group, jnp.where(lane == j + k, 1.0, 0.0), jnp.broadcast_to(home[k : k + 1, :], (8, size)))
            for k in range(GROUP)
        ]
        pivots = sweep(
            [[jnp.broadcast_to(spread[m][k : k + 1, :], (8, size)) for m in range(k + 1)] for k in range(GROUP)]
        )
        scaled = []
        for k in range(GROUP):
            terms = [pivots[k][m] * rows[m] for m in range(GROUP)]
            while len(terms) > 1:
                terms = [terms[i] + terms[i + 1] for i in range(0, len(terms), 2)]
            scaled.append(terms[0])
        nxt = []
        for t, tile in enumerate(tiles):
            if t == g:
                new = scaled[0]
                for k in range(1, GROUP):
                    new = jnp.where(sub == k, scaled[k], new)
            else:
                terms = [jnp.broadcast_to(tile[:, j + k : j + k + 1], (8, size)) * scaled[k] for k in range(GROUP)]
                while len(terms) > 1:
                    terms = [terms[i] + terms[i + 1] for i in range(0, len(terms), 2)]
                new = jnp.where(in_group, 0.0, tile) - terms[0]
            nxt.append(new)
        tiles = nxt
    return jnp.concatenate(tiles, axis=0)


def inverse_kernel(gram_ref, work, row, column):
    total = gram_ref.shape[0]
    size = BLOCK
    count = total // size
    scale = 1.0 / jnp.max(gram_ref[...])
    work[...] = gram_ref[...] * scale
    row[...] = jnp.zeros_like(row)
    column[...] = jnp.zeros_like(column)

    def step(k, carry):
        at = pl.ds(pl.multiple_of(k * size, size), size)
        inv = invert_block(work[at, at])
        for i in range(1, count):
            rows = pl.ds(pl.multiple_of(lax.rem(k + i, count) * size, size), size)
            work[rows, :] = work[rows, :] - precise_dot(column[rows, :], row[...])
        new = precise_dot(inv, work[at, :])
        for i in range(1, count):
            rows = pl.ds(pl.multiple_of(lax.rem(k + i, count) * size, size), size)
            column[rows, :] = work[rows, at]
            work[rows, at] = jnp.zeros((size, size), F32)
        work[at, :] = new
        work[at, at] = inv
        row[...] = new
        row[:, at] = inv
        soon = pl.ds(pl.multiple_of(lax.rem(k + 1, count) * size, size), size)
        work[soon, :] = work[soon, :] - precise_dot(column[soon, :], row[...])
        column[soon, :] = jnp.zeros((size, size), F32)
        column[at, :] = jnp.zeros((size, size), F32)
        return carry

    lax.fori_loop(0, count, step, 0)
    for i in range(count):
        rows = pl.ds(i * size, size)
        work[rows, :] = (work[rows, :] - precise_dot(column[rows, :], row[...])) * scale


def inverse_of(gram):
    total = gram.shape[0]
    return pl.pallas_call(
        inverse_kernel,
        out_shape=jax.ShapeDtypeStruct((total, total), F32),
        in_specs=[VMEM],
        out_specs=VMEM,
        scratch_shapes=[pltpu.VMEM((BLOCK, total), F32), pltpu.VMEM((total, BLOCK), F32)],
        compiler_params=pltpu.CompilerParams(vmem_limit_bytes=16 * 2**20),
        cost_estimate=pl.CostEstimate(flops=2 * 10**10, bytes_accessed=2 * 2**20, transcendentals=0),
        name="inverse",
    )(gram)


def last_kernel(gram_ref, rhs_ref, right_ref, first_ref, direction_ref, out_ref, work, row, column):
    total, cols = rhs_ref.shape
    size = BLOCK
    count = total // size
    scale = 1.0 / jnp.max(gram_ref[...])
    work[:, :total] = gram_ref[...] * scale
    work[:, total:] = rhs_ref[...] * scale
    row[...] = jnp.zeros_like(row)
    column[...] = jnp.zeros_like(column)
    out_ref[...] = dot_halves(halves(right_ref[...]), halves(first_ref[...]))

    def step(k, carry):
        at = pl.ds(pl.multiple_of(k * size, size), size)
        inv = invert_block(work[at, at])
        for i in range(1, count):
            rows = pl.ds(pl.multiple_of(lax.rem(k + i, count) * size, size), size)
            work[rows, :] = work[rows, :] - precise_dot(column[rows, :], row[...])
        new = precise_dot(inv, work[at, :])
        for i in range(1, count):
            rows = pl.ds(pl.multiple_of(lax.rem(k + i, count) * size, size), size)
            column[rows, :] = work[rows, at]
        work[at, :] = new
        row[...] = new
        soon = pl.ds(pl.multiple_of(lax.rem(k + 1, count) * size, size), size)
        work[soon, :] = work[soon, :] - precise_dot(column[soon, :], row[...])
        column[soon, :] = jnp.zeros((size, size), F32)
        column[at, :] = jnp.zeros((size, size), F32)
        return carry

    lax.fori_loop(0, count, step, 0)
    for i in range(count):
        rows = pl.ds(i * size, size)
        work[rows, total:] = work[rows, total:] - precise_dot(column[rows, :], row[:, total:])
    out_ref[...] += dot_halves(halves(direction_ref[...]), halves(work[:, total:]))


def last_solve(gram, rhs, right_all, first, direction):
    total, cols = rhs.shape
    return pl.pallas_call(
        last_kernel,
        out_shape=jax.ShapeDtypeStruct((direction.shape[0], cols), F32),
        in_specs=[VMEM] * 5,
        out_specs=VMEM,
        scratch_shapes=[
            pltpu.VMEM((total, total + cols), F32),
            pltpu.VMEM((BLOCK, total + cols), F32),
            pltpu.VMEM((total, BLOCK), F32),
        ],
        compiler_params=pltpu.CompilerParams(vmem_limit_bytes=24 * 2**20),
        cost_estimate=pl.CostEstimate(flops=2 * 10**10, bytes_accessed=3 * 2**20, transcendentals=0),
        name="last",
    )(gram, rhs, right_all, first, direction)


class Place:
    def __init__(self, n, groups):
        self.n, self.groups, self.lines = n, groups, n // PLANE
        self.me, self.col = lax.axis_index("samp"), lax.axis_index("tgt")
        self.inner = lax.rem(self.me, PLANE)
        self.line = lax.div(self.me, PLANE)
        self.over_x = self.me + 1 - 2 * lax.rem(self.me, 2)
        self.over_y = self.me + 2 - 4 * lax.div(self.inner, 2)
        self.inner_x = lax.rem(self.over_x, PLANE)
        self.inner_y = lax.rem(self.over_y, PLANE)
        self.along = [lax.rem(self.line + s, self.lines) * PLANE + self.inner for s in range(1, self.lines)]
        self.others = [lax.rem(self.col + s, groups) for s in range(1, groups)]

    def greet(self):
        barrier = pltpu.get_barrier_semaphore()
        for peer in [*self.along, self.over_x, self.over_y]:
            pl.semaphore_signal(barrier, inc=1, device_id={"samp": peer}, device_id_type=MESH)
        for other in self.others:
            pl.semaphore_signal(barrier, inc=1, device_id={"tgt": other}, device_id_type=MESH)

    def meet(self):
        pl.semaphore_wait(pltpu.get_barrier_semaphore(), len(self.along) + 2 + len(self.others))

    def behind(self, s, inner):
        return lax.rem(self.line + self.lines - s, self.lines) * PLANE + inner


class Gather:
    def __init__(self, place, slab, rows, sends, recvs):
        self.place, self.slab, self.rows, self.sends, self.recvs = place, slab, rows, sends, recvs
        self.started, self.mirrors = [], {}
        self.z, self.x, self.y, self.d = {}, {}, {}, {}

    def span(self, block, part=None):
        if part is None:
            return self.slab.at[pl.ds(pl.multiple_of(block * self.rows, self.rows), self.rows)]
        half = self.rows // 2
        return self.slab.at[pl.ds(pl.multiple_of(block * self.rows + part * half, half), half)]

    def send(self, ref, slot, peer):
        copy = pltpu.make_async_remote_copy(
            src_ref=ref,
            dst_ref=ref,
            send_sem=self.sends.at[slot],
            recv_sem=self.recvs.at[slot],
            device_id={"samp": peer},
            device_id_type=MESH,
        )
        copy.start()
        self.started.append(copy)
        return copy

    def across(self, s):
        p = self.place
        ref = self.span(p.behind(s, p.inner))
        base = p.lines + 4 * s
        self.x[s] = self.send(ref, base, p.over_x)
        self.y[s] = self.send(ref, base + 1, p.over_y)

    def along(self):
        p = self.place
        for s in range(1, p.lines):
            self.z[s] = self.send(self.span(p.me), s, p.along[s - 1])

    def open(self):
        self.along()
        self.across(0)

    def relay(self, s):
        self.z[s].wait_recv()
        self.across(s)

    def corner(self, s):
        p = self.place
        base = p.lines + 4 * s
        self.x[s].wait_recv()
        one = self.send(self.span(p.behind(s, p.inner_x), 0), base + 2, p.over_y)
        self.y[s].wait_recv()
        self.d[s] = [one, self.send(self.span(p.behind(s, p.inner_y), 1), base + 3, p.over_x)]

    def line(self, s):
        size = PLANE * self.rows
        first = lax.rem(self.place.line + self.place.lines - s, self.place.lines)
        return pl.ds(pl.multiple_of(first * size, size), size)

    def finish(self, s, mirror=None):
        for copy in self.d[s]:
            copy.wait_recv()
        if mirror is not None:
            sends, recvs, base = mirror
            ref = self.slab.at[self.line(s)]
            self.mirrors[s] = Swap(self.place, ref, ref, sends, recvs, base + s * self.place.groups)

    def actions(self, mirror=None):
        steps, lines = [], self.place.lines
        for s in range(1, lines):
            steps.append(functools.partial(self.relay, s))
            steps.append(functools.partial(self.corner, s - 1))
            if mirror is not None and s > 1:
                steps.append(functools.partial(self.finish, s - 2, mirror))
        steps.append(functools.partial(self.corner, lines - 1))
        if mirror is not None:
            for s in range(max(lines - 2, 0), lines):
                steps.append(functools.partial(self.finish, s, mirror))
        return steps

    def close(self):
        for s in range(self.place.lines):
            self.finish(s)

    def drain(self):
        for copy in self.started:
            copy.wait_send()
        for swap in self.mirrors.values():
            swap.drain()


def room(groups):
    return (63 if groups > 2 else 40) * 2**20


def slots(n):
    return n // PLANE + 4 * (n // PLANE)


class Swap:
    def __init__(self, place, src, dst, sends, recvs, base, slotted=False):
        self.copies = []
        for i, other in enumerate(place.others):
            copy = pltpu.make_async_remote_copy(
                src_ref=src,
                dst_ref=dst.at[i] if slotted else dst,
                send_sem=sends.at[base + i],
                recv_sem=recvs.at[base + i],
                device_id={"tgt": other},
                device_id_type=MESH,
            )
            copy.start()
            self.copies.append(copy)

    def wait(self):
        for copy in self.copies:
            copy.wait_recv()

    def drain(self):
        for copy in self.copies:
            copy.wait_send()


def interleave(actions, work, lead=0):
    done = min(lead, len(actions))
    for act in actions[:done]:
        act()
    rest = len(actions) - done
    for i, piece in enumerate(work):
        upto = len(actions) - rest + (i + 1) * rest // len(work)
        piece()
        for act in actions[done:upto]:
            act()
        done = upto


def beside(parts):
    return parts[0] if len(parts) == 1 else jnp.concatenate(parts, axis=1)


def first_kernel(
    n, groups, total_n,
    samples_hbm, omega_hbm, phase_hbm, right_hbm,
    gram_ref, mixed_ref, lifted_ref, part_ref, proj_ref, feats_ref, wide_ref,
    samples_ref, omega_ref, phase_ref, wides, spots, flat, rights, projs, lifts,
    loads, g_sends, g_recvs, s_sends, s_recvs, m_sends, m_recvs,
):
    place = Place(n, groups)
    me, col = place.me, place.col
    rows, depth = samples_ref.shape
    feats, cols = wides.shape[1:]
    total_f = omega_ref.shape[1]
    mine = total_f // groups
    pieces, piece = spots.shape[0], spots.shape[1] // n
    slab = col if pieces > 1 else 0

    fetches = [
        pltpu.make_async_copy(src, dst, loads.at[i])
        for i, (src, dst) in enumerate(
            [(samples_hbm, samples_ref), (right_hbm, wides.at[col]), (omega_hbm, omega_ref), (phase_hbm, phase_ref)]
        )
    ]
    for fetch in fetches:
        fetch.start()
    place.greet()
    fetches[0].wait()
    spots[slab, pl.ds(pl.multiple_of(me * piece, piece), piece), :] = samples_ref[
        pl.ds(pl.multiple_of(slab * piece, piece), piece), :
    ]
    fetches[1].wait()
    rights[col, pl.ds(pl.multiple_of(me * feats, feats), feats), :] = wides[col].astype(BF16)
    fetches[2].wait()
    fetches[3].wait()

    tile = 256

    def own_features(i, carry):
        at = pl.ds(pl.multiple_of(i * tile, tile), tile)
        feats_ref[:, at] = cosine(dot(samples_ref[...], omega_ref[:, at]) + phase_ref[:, at]).astype(BF16)
        return carry

    lax.fori_loop(0, total_f // tile, own_features, 0)
    place.meet()
    near = Gather(place, spots.at[slab], piece, g_sends.at[0], g_recvs.at[0])
    far = Gather(place, rights.at[col], feats, g_sends.at[1], g_recvs.at[1])
    near.open()
    far.open()
    swaps = [Swap(place, wides.at[col], wides.at[col], s_sends, s_recvs, 0)]
    for act in near.actions():
        act()
    near.close()
    if pieces > 1:
        swaps.append(Swap(place, spots.at[col], spots.at[col], s_sends, s_recvs, groups))
        swaps[-1].wait()

    def settle(b, carry):
        for t in range(pieces):
            flat[pl.ds(pl.multiple_of(b * rows + t * piece, piece), piece), :] = spots[
                t, pl.ds(pl.multiple_of(b * piece, piece), piece), :
            ]
        return carry

    lax.fori_loop(0, n, settle, 0)

    tiles = total_n // tile
    batch = 3 if tiles % 3 == 0 else 1

    def lift_features(c):
        at = pl.ds(pl.multiple_of(col * mine + c * tile, tile), tile)
        weights = omega_ref[:, at].T
        shift = jnp.broadcast_to(phase_ref[:, at], (128, tile)).T
        shift = jnp.concatenate([shift] * (tile // 128), axis=1)
        down = pl.ds(c * tile, tile)

        def one(i, carry):
            for b in range(batch):
                over = pl.ds(pl.multiple_of((i * batch + b) * tile, tile), tile)
                lifts[down, over] = cosine(dot(weights, flat[over, :], NT) + shift).astype(BF16)
            return carry

        lax.fori_loop(0, tiles // batch, one, 0)

    work = [functools.partial(lift_features, c) for c in range(mine // tile)]
    early = len(work) * 5 // 8
    interleave(far.actions(), work[:early], 3)
    far.close()
    spread = Swap(place, rights.at[col], rights.at[col], s_sends, s_recvs, 2 * groups)
    swaps.append(spread)
    projs[col, pl.ds(pl.multiple_of(me * rows, rows), rows), :] = dot(feats_ref[...], rights[col]).astype(BF16)
    last = Gather(place, projs.at[col], rows, g_sends.at[2], g_recvs.at[2])
    last.open()

    chunk = 512

    def gram_piece(lo, hi):
        def one(i, carry):
            at = pl.ds(pl.multiple_of(i * chunk, chunk), chunk)
            block = beside([rights[t, at, :] for t in range(groups)])
            gram_ref[...] += dot(block, block, TN)
            return carry

        lax.fori_loop(lo, hi, one, 0)

    gram_ref[...] = jnp.zeros_like(gram_ref)
    count = total_f // chunk
    steps = last.actions((m_sends, m_recvs, 0))
    ready = min(place.lines, PLANE) - 1
    mixed_ref[...] = jnp.zeros_like(mixed_ref)

    def absorb(s):
        block = beside([projs[t, last.line(s), :] for t in range(groups)])
        mixed_ref[...] += dot(block, block, TN)

    def lift(s, fresh):
        def one(i, carry):
            at = pl.ds(pl.multiple_of(i * chunk, chunk), chunk)
            left = lifts[at, last.line(s)]
            for t in range(groups):
                value = dot(left, projs[t, last.line(s), :]) * (1.0 / total_n)
                lifted_ref[t, at, :] = value if fresh else lifted_ref[t, at, :] + value
            return carry

        lax.fori_loop(0, mine // chunk, one, 0)

    grams = [functools.partial(gram_piece, i * count // 4, (i + 1) * count // 4) for i in range(4)]
    interleave(steps[:-2], [*work[early:], spread.wait, *grams])
    used = 0
    for act in [*steps[-2:], lambda: None]:
        if used < ready and used in last.mirrors:
            last.mirrors[used].wait()
            absorb(used)
            lift(used, used == 0)
            used += 1
        act()
    for s in range(used, place.lines):
        last.mirrors[s].wait()
    if place.lines - used <= PLANE:
        for s in range(used, place.lines):
            absorb(s)
            lift(s, s == 0)
    else:
        def rest(s, carry):
            absorb(s)
            lift(s, False)
            return carry

        lax.fori_loop(used, place.lines, rest, 0)
    mixed_ref[...] = mixed_ref[...] * (1.0 / total_n) + ridge * gram_ref[...]

    own = pl.ds(pl.multiple_of(me * rows, rows), rows)
    swaps[0].wait()
    for t in range(groups):
        part_ref[t] = rights[t, pl.ds(pl.multiple_of(col * mine, mine), mine), :]
        proj_ref[:, t * cols : (t + 1) * cols] = projs[t, own, :]
        wide_ref[:, t * cols : (t + 1) * cols] = wides[t]
    for gather in (near, far, last):
        gather.drain()
    for swap in swaps:
        swap.drain()


def first_stage(samples, omega, phase, right_side):
    n, groups = lax.axis_size("samp"), lax.axis_size("tgt")
    rows, depth = samples.shape
    feats, cols = right_side.shape
    total_f = omega.shape[1]
    total_n, mine, targets = rows * n, total_f // groups, cols * groups
    pieces = groups if rows % (32 * groups) == 0 else 1
    return pl.pallas_call(
        functools.partial(first_kernel, n, groups, total_n),
        out_shape=[
            jax.ShapeDtypeStruct((targets, targets), F32),
            jax.ShapeDtypeStruct((targets, targets), F32),
            jax.ShapeDtypeStruct((groups, mine, cols), F32),
            jax.ShapeDtypeStruct((groups, mine, cols), BF16),
            jax.ShapeDtypeStruct((rows, targets), BF16),
            jax.ShapeDtypeStruct((rows, total_f), BF16),
            jax.ShapeDtypeStruct((feats, targets), F32),
        ],
        in_specs=[pl.BlockSpec(memory_space=pltpu.HBM)] * 4,
        out_specs=[VMEM] * 7,
        scratch_shapes=[
            pltpu.VMEM((rows, depth), BF16),
            pltpu.VMEM((depth, total_f), BF16),
            pltpu.VMEM((1, total_f), F32),
            pltpu.VMEM((groups, feats, cols), F32),
            pltpu.VMEM((pieces, total_n // pieces, depth), BF16),
            pltpu.VMEM((total_n, depth), BF16),
            pltpu.VMEM((groups, total_f, cols), BF16),
            pltpu.VMEM((groups, total_n, cols), BF16),
            pltpu.VMEM((mine, total_n), BF16),
            pltpu.SemaphoreType.DMA((4,)),
            pltpu.SemaphoreType.DMA((3, slots(n))),
            pltpu.SemaphoreType.DMA((3, slots(n))),
            pltpu.SemaphoreType.DMA((3 * groups,)),
            pltpu.SemaphoreType.DMA((3 * groups,)),
            pltpu.SemaphoreType.DMA((n // PLANE * groups,)),
            pltpu.SemaphoreType.DMA((n // PLANE * groups,)),
        ],
        compiler_params=pltpu.CompilerParams(collective_id=0, has_side_effects=True, vmem_limit_bytes=room(groups)),
        cost_estimate=pl.CostEstimate(flops=10**11, bytes_accessed=2 * 2**20, transcendentals=0),
        name="first",
    )(samples, omega, phase.reshape(1, -1), right_side)


def second_kernel(
    n, groups, total_n,
    inverse_ref, gram_ref, lifted_ref, part_ref, proj_ref, feats_ref,
    first_ref, target_ref, final_ref, direction_ref,
    resid, sums, theirs, aside, away, projs, shared, g_sends, g_recvs, s_sends, s_recvs, m_sends, m_recvs,
):
    place = Place(n, groups)
    me, col = place.me, place.col
    rows = feats_ref.shape[0]
    mine, cols = lifted_ref.shape[1:]
    targets = groups * cols
    chunk = 512
    place.greet()
    inverse = halves(inverse_ref[...])
    alpha = dot_halves(inverse, halves(gram_ref[...]))
    alpha_halves = halves(alpha)
    for t in range(groups):
        pl.when(col == t)(functools.partial(first_ref.__setitem__, Ellipsis, alpha[:, t * cols : (t + 1) * cols]))
    sums[...] = jnp.zeros_like(sums)
    aside[...] = jnp.zeros_like(aside)

    def one(i, carry):
        at = pl.ds(pl.multiple_of(i * chunk, chunk), chunk)
        right = beside([part_ref[t, at, :] for t in range(groups)]).astype(F32)
        image = halves(beside([lifted_ref[t, at, :] for t in range(groups)]) + ridge * right)
        left = right - dot_halves(image, alpha_halves)
        resid[at, :] = left
        pair = halves(left)
        sums[0] += dot_halves(image, pair, TN)
        over = pl.ds(pl.multiple_of(col * mine + i * chunk, chunk), chunk)
        aside[...] += dot(feats_ref[:, over], pair[0])
        return carry

    lax.fori_loop(0, mine // chunk, one, 0)
    place.meet()
    swaps = [
        Swap(place, sums.at[0], theirs.at[0], s_sends, s_recvs, 0, True),
        Swap(place, aside, away, s_sends, s_recvs, groups, True),
    ]
    swaps[0].wait()

    def total(which):
        value = sums[which]
        for i in range(groups - 1):
            value = value + theirs[which, i]
        return value

    beta = -dot_halves(inverse, halves(total(0)))
    beta_halves = halves(beta)
    swaps[1].wait()
    value = aside[...]
    for i in range(groups - 1):
        value = value + away[i]
    value = value + dot(proj_ref[...], beta_halves[0]) + dot(proj_ref[...], beta_halves[1])
    own = pl.ds(pl.multiple_of(me * rows, rows), rows)
    for t in range(groups):
        pl.when(col == t)(
            functools.partial(projs.__setitem__, (t, own), value[:, t * cols : (t + 1) * cols].astype(BF16))
        )
    gather = Gather(place, projs.at[col], rows, g_sends, g_recvs)
    gather.open()
    final_ref[...] = jnp.zeros_like(final_ref)

    def turn(i):
        at = pl.ds(i * chunk, chunk)
        right = beside([part_ref[t, at, :] for t in range(groups)])
        left = resid[at, :]
        pair = halves(left)
        sums[1] += dot_halves(pair, pair, TN)
        line = left + dot(right, beta_halves[0]) + dot(right, beta_halves[1])
        resid[at, :] = line
        pair = halves(line)
        final_ref[...] += dot_halves(pair, pair, TN)

    turns = [functools.partial(turn, i) for i in range(mine // chunk)]
    steps = gather.actions((m_sends, m_recvs, 0))
    cut = len(steps) * 2 // 3
    interleave(steps[:cut], turns)
    swaps.append(Swap(place, final_ref, shared, s_sends, s_recvs, 3 * groups, True))
    swaps.append(Swap(place, sums.at[1], theirs.at[1], s_sends, s_recvs, 2 * groups, True))
    feats = direction_ref.shape[0]
    owners = n // groups
    source = lax.div(me, owners)
    held = pl.ds(pl.multiple_of(lax.rem(me, owners) * feats, feats), feats)

    def copies():
        return [
            pltpu.make_async_remote_copy(
                src_ref=resid.at[held],
                dst_ref=resid.at[pl.ds(mine, feats)],
                send_sem=s_sends.at[4 * groups + i],
                recv_sem=s_recvs.at[4 * groups],
                device_id={"tgt": other},
                device_id_type=MESH,
            )
            for i, other in enumerate(place.others)
        ]

    @pl.when(col == source)
    def _():
        for copy in copies():
            copy.start()

    steps[cut]()
    swaps[2].wait()
    swaps[2].drain()
    value = final_ref[...]
    for i in range(groups - 1):
        value = value + shared[i]
    final_ref[...] = ridge * value

    def mix(s):
        block = beside([projs[t, gather.line(s), :] for t in range(groups)])
        final_ref[...] += dot(block, block, TN) * (1.0 / total_n)

    mixed = 0
    for act in steps[cut + 1 :]:
        act()
        while mixed < min(place.lines, PLANE) - 2 and mixed in gather.mirrors:
            gather.mirrors[mixed].wait()
            mix(mixed)
            mixed += 1
    swaps[3].wait()
    new = total(1)
    for t in range(groups):
        pl.when(col == t)(functools.partial(target_ref.__setitem__, Ellipsis, new[:, t * cols : (t + 1) * cols]))
    for s in range(mixed, place.lines):
        gather.mirrors[s].wait()
    if place.lines - mixed <= PLANE:
        for s in range(mixed, place.lines):
            mix(s)
    else:
        def rest(s, carry):
            mix(s)
            return carry

        lax.fori_loop(mixed, place.lines, rest, 0)

    @pl.when(col == source)
    def _():
        direction_ref[...] = resid[held, :]
        for copy in copies():
            copy.wait_send()

    @pl.when(col != source)
    def _():
        copies()[0].wait_recv()
        direction_ref[...] = resid[pl.ds(mine, feats), :]

    gather.drain()
    for swap in swaps[:2] + swaps[3:]:
        swap.drain()


def second_stage(inverse, gram, lifted, part, proj, feats_own, feats):
    n, groups = lax.axis_size("samp"), lax.axis_size("tgt")
    _, mine, cols = lifted.shape
    rows = feats_own.shape[0]
    total_n, targets = rows * n, cols * groups
    return pl.pallas_call(
        functools.partial(second_kernel, n, groups, total_n),
        out_shape=[
            jax.ShapeDtypeStruct((targets, cols), F32),
            jax.ShapeDtypeStruct((targets, cols), F32),
            jax.ShapeDtypeStruct((targets, targets), F32),
            jax.ShapeDtypeStruct((feats, targets), F32),
        ],
        in_specs=[VMEM] * 6,
        out_specs=[VMEM] * 4,
        scratch_shapes=[
            pltpu.VMEM((mine + feats, targets), F32),
            pltpu.VMEM((2, targets, targets), F32),
            pltpu.VMEM((2, max(groups - 1, 1), targets, targets), F32),
            pltpu.VMEM((rows, targets), F32),
            pltpu.VMEM((max(groups - 1, 1), rows, targets), F32),
            pltpu.VMEM((groups, total_n, cols), BF16),
            pltpu.VMEM((max(groups - 1, 1), targets, targets), F32),
            pltpu.SemaphoreType.DMA((slots(n),)),
            pltpu.SemaphoreType.DMA((slots(n),)),
            pltpu.SemaphoreType.DMA((5 * groups,)),
            pltpu.SemaphoreType.DMA((5 * groups,)),
            pltpu.SemaphoreType.DMA((n // PLANE * groups,)),
            pltpu.SemaphoreType.DMA((n // PLANE * groups,)),
        ],
        compiler_params=pltpu.CompilerParams(collective_id=1, has_side_effects=True, vmem_limit_bytes=room(groups)),
        cost_estimate=pl.CostEstimate(flops=10**11, bytes_accessed=2 * 2**20, transcendentals=0),
        name="second",
    )(inverse, gram, lifted, part, proj, feats_own)


def body(samples, omega, phase, right_side):
    gram, mixed, lifted, part, proj, feats_own, right_all = first_stage(samples, omega, phase, right_side)
    inverse = inverse_of(mixed)
    first, target, final, direction = second_stage(
        inverse, gram, lifted, part, proj, feats_own, right_side.shape[0]
    )
    return last_solve(final, target, right_all, first, direction)


def solution(mesh):
    placed = (P("samp", None), P(), P(), P("samp", "tgt"))
    return jax.shard_map(
        body, mesh=mesh, in_specs=placed, out_specs=P("samp", "tgt"), check_vma=False
    )
```

```python
import functools

import jax
import jax.numpy as jnp
from jax import lax
from jax.experimental import pallas as pl
from jax.experimental.pallas import tpu as pltpu
from jax.sharding import PartitionSpec as P

ridge = 1.0
HI = lax.Precision.HIGHEST
F32 = jnp.float32
BF16 = jnp.bfloat16
BLOCK = 128
GROUP = 8
PLANE = 4
MESH = pl.DeviceIdType.MESH
NN = (((1,), (0,)), ((), ()))
TN = (((0,), (0,)), ((), ()))
NT = (((1,), (1,)), ((), ()))
VMEM = pl.BlockSpec(memory_space=pltpu.VMEM)


def precise_dot(left_matrix, right_matrix):
    return jnp.dot(left_matrix, right_matrix, precision=HI, preferred_element_type=F32)


def dot(left, right, dims=NN):
    return lax.dot_general(left, right, dims, preferred_element_type=F32)


def halves(x):
    high = x.astype(BF16)
    return high, (x - high.astype(F32)).astype(BF16)


def dot_halves(left, right, dims=NN):
    return dot(left[0], right[0], dims) + (dot(left[0], right[1], dims) + dot(left[1], right[0], dims))


def cosine(x):
    turns = x * 0.15915494309189535
    f = turns - jnp.round(turns)
    s = f * f
    p = -21.071105627575776
    for coef in (
        58.790492120100176,
        -85.27162153429538,
        64.92865742103322,
        -19.738980355764014,
        0.999999210782322,
    ):
        p = p * s + coef
    return p


def sweep(held):
    size = len(held)
    at = lambda i, j: held[max(i, j)][min(i, j)]
    for p in range(0, size, 2):
        q = p + 1
        a, b, c = held[p][p], held[q][p], held[q][q]
        scale = 1.0 / (a * c - b * b)
        pp, pq, qq = c * scale, b * scale, a * scale
        first, second = [at(i, p) for i in range(size)], [at(i, q) for i in range(size)]
        rest = [i for i in range(size) if i not in (p, q)]
        left = {i: first[i] * pp - second[i] * pq for i in rest}
        right = {i: second[i] * qq - first[i] * pq for i in rest}
        for i in rest:
            for j in rest:
                if j <= i:
                    held[i][j] = held[i][j] - (left[i] * first[j] + right[i] * second[j])
        for i in rest:
            held[max(i, p)][min(i, p)] = left[i]
            held[max(i, q)][min(i, q)] = right[i]
        held[p][p], held[q][p], held[q][q] = -pp, pq, -qq
    return [[-at(i, j) for j in range(size)] for i in range(size)]


def invert_block(value, unit):
    size = value.shape[0]
    tiles = [value[t * 8 : t * 8 + 8, :] for t in range(size // 8)]
    lane = lax.broadcasted_iota(jnp.int32, (8, size), 1)
    sub = lax.broadcasted_iota(jnp.int32, (8, size), 0)
    for g in range(size // GROUP):
        j = g * GROUP
        in_group = (lane >= j) & (lane < j + GROUP)
        home = tiles[g]
        spread = [jnp.broadcast_to(home[:, j + m : j + m + 1], (8, size)) * unit for m in range(GROUP)]
        rows = [
            jnp.where(in_group, jnp.where(lane == j + k, 1.0, 0.0), jnp.broadcast_to(home[k : k + 1, :], (8, size)))
            for k in range(GROUP)
        ]
        pivots = sweep(
            [[jnp.broadcast_to(spread[m][k : k + 1, :], (8, size)) for m in range(k + 1)] for k in range(GROUP)]
        )
        scaled = []
        for k in range(GROUP):
            terms = [pivots[k][m] * rows[m] for m in range(GROUP)]
            while len(terms) > 1:
                terms = [terms[i] + terms[i + 1] for i in range(0, len(terms), 2)]
            scaled.append(terms[0])
        nxt = []
        for t, tile in enumerate(tiles):
            if t == g:
                new = scaled[0]
                for k in range(1, GROUP):
                    new = jnp.where(sub == k, scaled[k], new)
            else:
                terms = [jnp.broadcast_to(tile[:, j + k : j + k + 1], (8, size)) * scaled[k] for k in range(GROUP)]
                while len(terms) > 1:
                    terms = [terms[i] + terms[i + 1] for i in range(0, len(terms), 2)]
                new = jnp.where(in_group, 0.0, tile) - terms[0]
            nxt.append(new)
        tiles = nxt
    return jnp.concatenate(tiles, axis=0)


def inverse_kernel(gram_ref, work, row, column, ones):
    total = gram_ref.shape[0]
    size = BLOCK
    count = total // size
    scale = 1.0 / jnp.max(gram_ref[...])
    work[...] = gram_ref[...] * scale
    row[...] = jnp.zeros_like(row)
    column[...] = jnp.zeros_like(column)
    ones[...] = jnp.ones_like(ones)

    def step(k, carry):
        at = pl.ds(pl.multiple_of(k * size, size), size)
        inv = invert_block(work[at, at], ones[...])
        for i in range(1, count):
            rows = pl.ds(pl.multiple_of(lax.rem(k + i, count) * size, size), size)
            work[rows, :] = work[rows, :] - precise_dot(column[rows, :], row[...])
        new = precise_dot(inv, work[at, :])
        for i in range(1, count):
            rows = pl.ds(pl.multiple_of(lax.rem(k + i, count) * size, size), size)
            column[rows, :] = work[rows, at]
            work[rows, at] = jnp.zeros((size, size), F32)
        work[at, :] = new
        work[at, at] = inv
        row[...] = new
        row[:, at] = inv
        soon = pl.ds(pl.multiple_of(lax.rem(k + 1, count) * size, size), size)
        work[soon, :] = work[soon, :] - precise_dot(column[soon, :], row[...])
        column[soon, :] = jnp.zeros((size, size), F32)
        column[at, :] = jnp.zeros((size, size), F32)
        return carry

    lax.fori_loop(0, count, step, 0)
    for i in range(count):
        rows = pl.ds(i * size, size)
        work[rows, :] = (work[rows, :] - precise_dot(column[rows, :], row[...])) * scale


def inverse_of(gram):
    total = gram.shape[0]
    return pl.pallas_call(
        inverse_kernel,
        out_shape=jax.ShapeDtypeStruct((total, total), F32),
        in_specs=[VMEM],
        out_specs=VMEM,
        scratch_shapes=[
            pltpu.VMEM((BLOCK, total), F32),
            pltpu.VMEM((total, BLOCK), F32),
            pltpu.VMEM((8, BLOCK), F32),
        ],
        compiler_params=pltpu.CompilerParams(vmem_limit_bytes=16 * 2**20),
        cost_estimate=pl.CostEstimate(flops=2 * 10**10, bytes_accessed=2 * 2**20, transcendentals=0),
        name="inverse",
    )(gram)


def last_kernel(gram_ref, rhs_ref, right_ref, first_ref, direction_ref, out_ref, work, row, column, ones):
    total, cols = rhs_ref.shape
    size = BLOCK
    count = total // size
    scale = 1.0 / jnp.max(gram_ref[...])
    work[:, :total] = gram_ref[...] * scale
    work[:, total:] = rhs_ref[...] * scale
    row[...] = jnp.zeros_like(row)
    column[...] = jnp.zeros_like(column)
    ones[...] = jnp.ones_like(ones)
    out_ref[...] = dot_halves(halves(right_ref[...]), halves(first_ref[...]))

    def step(k, carry):
        at = pl.ds(pl.multiple_of(k * size, size), size)
        inv = invert_block(work[at, at], ones[...])
        for i in range(1, count):
            rows = pl.ds(pl.multiple_of(lax.rem(k + i, count) * size, size), size)
            work[rows, :] = work[rows, :] - precise_dot(column[rows, :], row[...])
        new = precise_dot(inv, work[at, :])
        for i in range(1, count):
            rows = pl.ds(pl.multiple_of(lax.rem(k + i, count) * size, size), size)
            column[rows, :] = work[rows, at]
        work[at, :] = new
        row[...] = new
        soon = pl.ds(pl.multiple_of(lax.rem(k + 1, count) * size, size), size)
        work[soon, :] = work[soon, :] - precise_dot(column[soon, :], row[...])
        column[soon, :] = jnp.zeros((size, size), F32)
        column[at, :] = jnp.zeros((size, size), F32)
        return carry

    lax.fori_loop(0, count, step, 0)
    for i in range(count):
        rows = pl.ds(i * size, size)
        work[rows, total:] = work[rows, total:] - precise_dot(column[rows, :], row[:, total:])
    out_ref[...] += dot_halves(halves(direction_ref[...]), halves(work[:, total:]))


def last_solve(gram, rhs, right_all, first, direction):
    total, cols = rhs.shape
    return pl.pallas_call(
        last_kernel,
        out_shape=jax.ShapeDtypeStruct((direction.shape[0], cols), F32),
        in_specs=[VMEM] * 5,
        out_specs=VMEM,
        scratch_shapes=[
            pltpu.VMEM((total, total + cols), F32),
            pltpu.VMEM((BLOCK, total + cols), F32),
            pltpu.VMEM((total, BLOCK), F32),
            pltpu.VMEM((8, BLOCK), F32),
        ],
        compiler_params=pltpu.CompilerParams(vmem_limit_bytes=24 * 2**20),
        cost_estimate=pl.CostEstimate(flops=2 * 10**10, bytes_accessed=3 * 2**20, transcendentals=0),
        name="last",
    )(gram, rhs, right_all, first, direction)


class Place:
    def __init__(self, n, groups):
        self.n, self.groups, self.lines = n, groups, n // PLANE
        self.me, self.col = lax.axis_index("samp"), lax.axis_index("tgt")
        self.inner = lax.rem(self.me, PLANE)
        self.line = lax.div(self.me, PLANE)
        self.over_x = self.me + 1 - 2 * lax.rem(self.me, 2)
        self.over_y = self.me + 2 - 4 * lax.div(self.inner, 2)
        self.inner_x = lax.rem(self.over_x, PLANE)
        self.inner_y = lax.rem(self.over_y, PLANE)
        self.along = [lax.rem(self.line + s, self.lines) * PLANE + self.inner for s in range(1, self.lines)]
        self.others = [lax.rem(self.col + s, groups) for s in range(1, groups)]

    def greet(self):
        barrier = pltpu.get_barrier_semaphore()
        for peer in [*self.along, self.over_x, self.over_y]:
            pl.semaphore_signal(barrier, inc=1, device_id={"samp": peer}, device_id_type=MESH)
        for other in self.others:
            pl.semaphore_signal(barrier, inc=1, device_id={"tgt": other}, device_id_type=MESH)

    def meet(self):
        pl.semaphore_wait(pltpu.get_barrier_semaphore(), len(self.along) + 2 + len(self.others))

    def behind(self, s, inner):
        return lax.rem(self.line + self.lines - s, self.lines) * PLANE + inner


class Gather:
    def __init__(self, place, slab, rows, sends, recvs):
        self.place, self.slab, self.rows, self.sends, self.recvs = place, slab, rows, sends, recvs
        self.started, self.mirrors = [], {}
        self.z, self.x, self.y, self.d = {}, {}, {}, {}

    def span(self, block, part=None):
        if part is None:
            return self.slab.at[pl.ds(pl.multiple_of(block * self.rows, self.rows), self.rows)]
        half = self.rows // 2
        return self.slab.at[pl.ds(pl.multiple_of(block * self.rows + part * half, half), half)]

    def send(self, ref, slot, peer):
        copy = pltpu.make_async_remote_copy(
            src_ref=ref,
            dst_ref=ref,
            send_sem=self.sends.at[slot],
            recv_sem=self.recvs.at[slot],
            device_id={"samp": peer},
            device_id_type=MESH,
        )
        copy.start()
        self.started.append(copy)
        return copy

    def across(self, s):
        p = self.place
        ref = self.span(p.behind(s, p.inner))
        base = p.lines + 4 * s
        self.x[s] = self.send(ref, base, p.over_x)
        self.y[s] = self.send(ref, base + 1, p.over_y)

    def along(self):
        p = self.place
        for s in range(1, p.lines):
            self.z[s] = self.send(self.span(p.me), s, p.along[s - 1])

    def open(self):
        self.along()
        self.across(0)

    def relay(self, s):
        self.z[s].wait_recv()
        self.across(s)

    def corner(self, s):
        p = self.place
        base = p.lines + 4 * s
        self.x[s].wait_recv()
        one = self.send(self.span(p.behind(s, p.inner_x), 0), base + 2, p.over_y)
        self.y[s].wait_recv()
        self.d[s] = [one, self.send(self.span(p.behind(s, p.inner_y), 1), base + 3, p.over_x)]

    def line(self, s):
        size = PLANE * self.rows
        first = lax.rem(self.place.line + self.place.lines - s, self.place.lines)
        return pl.ds(pl.multiple_of(first * size, size), size)

    def finish(self, s, mirror=None):
        for copy in self.d[s]:
            copy.wait_recv()
        if mirror is not None:
            sends, recvs, base = mirror
            ref = self.slab.at[self.line(s)]
            self.mirrors[s] = Swap(self.place, ref, ref, sends, recvs, base + s * self.place.groups)

    def actions(self, mirror=None):
        lines = self.place.lines
        steps = [functools.partial(self.corner, 0)]
        steps += [functools.partial(self.relay, s) for s in range(1, min(lines, 4))]
        for s in range(1, lines):
            steps.append(functools.partial(self.corner, s))
            if s + 3 < lines:
                steps.append(functools.partial(self.relay, s + 3))
            if mirror is not None:
                steps.append(functools.partial(self.finish, s - 1, mirror))
        if mirror is not None:
            steps.append(functools.partial(self.finish, lines - 1, mirror))
        return steps

    def close(self):
        for s in range(self.place.lines):
            self.finish(s)

    def drain(self):
        for copy in self.started:
            copy.wait_send()
        for swap in self.mirrors.values():
            swap.drain()


def room(groups):
    return (63 if groups > 2 else 40) * 2**20


def slots(n):
    return n // PLANE + 4 * (n // PLANE)


class Swap:
    def __init__(self, place, src, dst, sends, recvs, base, slotted=False):
        self.copies = []
        for i, other in enumerate(place.others):
            copy = pltpu.make_async_remote_copy(
                src_ref=src,
                dst_ref=dst.at[i] if slotted else dst,
                send_sem=sends.at[base + i],
                recv_sem=recvs.at[base + i],
                device_id={"tgt": other},
                device_id_type=MESH,
            )
            copy.start()
            self.copies.append(copy)

    def wait(self):
        for copy in self.copies:
            copy.wait_recv()

    def drain(self):
        for copy in self.copies:
            copy.wait_send()


def interleave(actions, work, lead=0):
    done = min(lead, len(actions))
    for act in actions[:done]:
        act()
    rest = len(actions) - done
    for i, piece in enumerate(work):
        upto = len(actions) - rest + (i + 1) * rest // len(work)
        piece()
        for act in actions[done:upto]:
            act()
        done = upto


def beside(parts):
    return parts[0] if len(parts) == 1 else jnp.concatenate(parts, axis=1)


def first_kernel(
    n, groups, total_n,
    samples_hbm, omega_hbm, phase_hbm, right_hbm,
    gram_ref, mixed_ref, lifted_ref, part_ref, proj_ref, feats_ref, wide_ref,
    samples_ref, omega_ref, phase_ref, wides, spots, flat, rights, projs, lifts,
    loads, g_sends, g_recvs, s_sends, s_recvs, m_sends, m_recvs,
):
    place = Place(n, groups)
    me, col = place.me, place.col
    rows, depth = samples_ref.shape
    feats, cols = wides.shape[1:]
    total_f = omega_ref.shape[1]
    mine = total_f // groups
    pieces, piece = spots.shape[0], spots.shape[1] // n
    slab = col if pieces > 1 else 0

    fetches = [
        pltpu.make_async_copy(src, dst, loads.at[i])
        for i, (src, dst) in enumerate(
            [(samples_hbm, samples_ref), (right_hbm, wides.at[col]), (omega_hbm, omega_ref), (phase_hbm, phase_ref)]
        )
    ]
    for fetch in fetches:
        fetch.start()
    place.greet()
    fetches[0].wait()
    spots[slab, pl.ds(pl.multiple_of(me * piece, piece), piece), :] = samples_ref[
        pl.ds(pl.multiple_of(slab * piece, piece), piece), :
    ]
    fetches[1].wait()
    rights[col, pl.ds(pl.multiple_of(me * feats, feats), feats), :] = wides[col].astype(BF16)
    fetches[2].wait()
    fetches[3].wait()

    tile = 256

    def own_features(i, carry):
        at = pl.ds(pl.multiple_of(i * tile, tile), tile)
        feats_ref[:, at] = cosine(dot(samples_ref[...], omega_ref[:, at]) + phase_ref[:, at]).astype(BF16)
        return carry

    lax.fori_loop(0, total_f // tile, own_features, 0)
    place.meet()
    near = Gather(place, spots.at[slab], piece, g_sends.at[0], g_recvs.at[0])
    far = Gather(place, rights.at[col], feats, g_sends.at[1], g_recvs.at[1])
    near.open()
    far.open()
    swaps = [Swap(place, wides.at[col], wides.at[col], s_sends, s_recvs, 0)]
    for act in near.actions():
        act()
    near.close()
    if pieces > 1:
        swaps.append(Swap(place, spots.at[col], spots.at[col], s_sends, s_recvs, groups))
        swaps[-1].wait()

    def settle(b, carry):
        for t in range(pieces):
            flat[pl.ds(pl.multiple_of(b * rows + t * piece, piece), piece), :] = spots[
                t, pl.ds(pl.multiple_of(b * piece, piece), piece), :
            ]
        return carry

    lax.fori_loop(0, n, settle, 0)

    tiles = total_n // tile
    batch = 3 if tiles % 3 == 0 else 1

    def lift_features(c):
        at = pl.ds(pl.multiple_of(col * mine + c * tile, tile), tile)
        weights = omega_ref[:, at].T
        shift = jnp.broadcast_to(phase_ref[:, at], (128, tile)).T
        shift = jnp.concatenate([shift] * (tile // 128), axis=1)
        down = pl.ds(c * tile, tile)

        def one(i, carry):
            for b in range(batch):
                over = pl.ds(pl.multiple_of((i * batch + b) * tile, tile), tile)
                lifts[down, over] = cosine(dot(weights, flat[over, :], NT) + shift).astype(BF16)
            return carry

        lax.fori_loop(0, tiles // batch, one, 0)

    work = [functools.partial(lift_features, c) for c in range(mine // tile)]
    early = len(work) * 5 // 8
    interleave(far.actions(), work[:early], 3)
    far.close()
    spread = Swap(place, rights.at[col], rights.at[col], s_sends, s_recvs, 2 * groups)
    swaps.append(spread)
    projs[col, pl.ds(pl.multiple_of(me * rows, rows), rows), :] = dot(feats_ref[...], rights[col]).astype(BF16)
    last = Gather(place, projs.at[col], rows, g_sends.at[2], g_recvs.at[2])
    last.open()

    chunk = 512

    def gram_piece(lo, hi):
        def one(i, carry):
            at = pl.ds(pl.multiple_of(i * chunk, chunk), chunk)
            block = beside([rights[t, at, :] for t in range(groups)])
            gram_ref[...] += dot(block, block, TN)
            return carry

        lax.fori_loop(lo, hi, one, 0)

    gram_ref[...] = jnp.zeros_like(gram_ref)
    count = total_f // chunk
    steps = last.actions((m_sends, m_recvs, 0))
    ready = min(place.lines, PLANE) - 1
    mixed_ref[...] = jnp.zeros_like(mixed_ref)

    def absorb(s):
        block = beside([projs[t, last.line(s), :] for t in range(groups)])
        mixed_ref[...] += dot(block, block, TN)

    def lift(s, fresh):
        def one(i, carry):
            at = pl.ds(pl.multiple_of(i * chunk, chunk), chunk)
            left = lifts[at, last.line(s)]
            for t in range(groups):
                value = dot(left, projs[t, last.line(s), :]) * (1.0 / total_n)
                lifted_ref[t, at, :] = value if fresh else lifted_ref[t, at, :] + value
            return carry

        lax.fori_loop(0, mine // chunk, one, 0)

    grams = [functools.partial(gram_piece, i * count // 4, (i + 1) * count // 4) for i in range(4)]
    interleave(steps[:-2], [*work[early:], spread.wait, *grams])
    used = 0
    for act in [*steps[-2:], lambda: None]:
        if used < ready and used in last.mirrors:
            last.mirrors[used].wait()
            absorb(used)
            lift(used, used == 0)
            used += 1
        act()
    for s in range(used, place.lines):
        last.mirrors[s].wait()
    if place.lines - used <= PLANE:
        for s in range(used, place.lines):
            absorb(s)
            lift(s, s == 0)
    else:
        def rest(s, carry):
            absorb(s)
            lift(s, False)
            return carry

        lax.fori_loop(used, place.lines, rest, 0)
    mixed_ref[...] = mixed_ref[...] * (1.0 / total_n) + ridge * gram_ref[...]

    own = pl.ds(pl.multiple_of(me * rows, rows), rows)
    swaps[0].wait()
    for t in range(groups):
        part_ref[t] = rights[t, pl.ds(pl.multiple_of(col * mine, mine), mine), :]
        proj_ref[:, t * cols : (t + 1) * cols] = projs[t, own, :]
        wide_ref[:, t * cols : (t + 1) * cols] = wides[t]
    for gather in (near, far, last):
        gather.drain()
    for swap in swaps:
        swap.drain()


def first_stage(samples, omega, phase, right_side):
    n, groups = lax.axis_size("samp"), lax.axis_size("tgt")
    rows, depth = samples.shape
    feats, cols = right_side.shape
    total_f = omega.shape[1]
    total_n, mine, targets = rows * n, total_f // groups, cols * groups
    pieces = groups if rows % (32 * groups) == 0 else 1
    return pl.pallas_call(
        functools.partial(first_kernel, n, groups, total_n),
        out_shape=[
            jax.ShapeDtypeStruct((targets, targets), F32),
            jax.ShapeDtypeStruct((targets, targets), F32),
            jax.ShapeDtypeStruct((groups, mine, cols), F32),
            jax.ShapeDtypeStruct((groups, mine, cols), BF16),
            jax.ShapeDtypeStruct((rows, targets), BF16),
            jax.ShapeDtypeStruct((rows, total_f), BF16),
            jax.ShapeDtypeStruct((feats, targets), F32),
        ],
        in_specs=[pl.BlockSpec(memory_space=pltpu.HBM)] * 4,
        out_specs=[VMEM] * 7,
        scratch_shapes=[
            pltpu.VMEM((rows, depth), BF16),
            pltpu.VMEM((depth, total_f), BF16),
            pltpu.VMEM((1, total_f), F32),
            pltpu.VMEM((groups, feats, cols), F32),
            pltpu.VMEM((pieces, total_n // pieces, depth), BF16),
            pltpu.VMEM((total_n, depth), BF16),
            pltpu.VMEM((groups, total_f, cols), BF16),
            pltpu.VMEM((groups, total_n, cols), BF16),
            pltpu.VMEM((mine, total_n), BF16),
            pltpu.SemaphoreType.DMA((4,)),
            pltpu.SemaphoreType.DMA((3, slots(n))),
            pltpu.SemaphoreType.DMA((3, slots(n))),
            pltpu.SemaphoreType.DMA((3 * groups,)),
            pltpu.SemaphoreType.DMA((3 * groups,)),
            pltpu.SemaphoreType.DMA((n // PLANE * groups,)),
            pltpu.SemaphoreType.DMA((n // PLANE * groups,)),
        ],
        compiler_params=pltpu.CompilerParams(collective_id=0, has_side_effects=True, vmem_limit_bytes=room(groups)),
        cost_estimate=pl.CostEstimate(flops=10**11, bytes_accessed=2 * 2**20, transcendentals=0),
        name="first",
    )(*[pltpu.with_memory_space_constraint(x, pltpu.HBM) for x in (samples, omega, phase.reshape(1, -1), right_side)])


def second_kernel(
    n, groups, total_n,
    inverse_ref, gram_ref, lifted_ref, part_ref, proj_ref, feats_ref,
    first_ref, target_ref, final_ref, direction_ref,
    resid, sums, theirs, aside, away, projs, shared, g_sends, g_recvs, s_sends, s_recvs, m_sends, m_recvs,
):
    place = Place(n, groups)
    me, col = place.me, place.col
    rows = feats_ref.shape[0]
    mine, cols = lifted_ref.shape[1:]
    targets = groups * cols
    chunk = 512
    place.greet()
    inverse = halves(inverse_ref[...])
    alpha = dot_halves(inverse, halves(gram_ref[...]))
    alpha_halves = halves(alpha)
    for t in range(groups):
        pl.when(col == t)(functools.partial(first_ref.__setitem__, Ellipsis, alpha[:, t * cols : (t + 1) * cols]))
    sums[...] = jnp.zeros_like(sums)
    aside[...] = jnp.zeros_like(aside)

    def one(i, carry):
        at = pl.ds(pl.multiple_of(i * chunk, chunk), chunk)
        right = beside([part_ref[t, at, :] for t in range(groups)]).astype(F32)
        image = halves(beside([lifted_ref[t, at, :] for t in range(groups)]) + ridge * right)
        left = right - dot_halves(image, alpha_halves)
        resid[at, :] = left
        pair = halves(left)
        sums[0] += dot_halves(image, pair, TN)
        over = pl.ds(pl.multiple_of(col * mine + i * chunk, chunk), chunk)
        aside[...] += dot(feats_ref[:, over], pair[0])
        return carry

    lax.fori_loop(0, mine // chunk, one, 0)
    place.meet()
    swaps = [
        Swap(place, sums.at[0], theirs.at[0], s_sends, s_recvs, 0, True),
        Swap(place, aside, away, s_sends, s_recvs, groups, True),
    ]
    swaps[0].wait()

    def total(which):
        value = sums[which]
        for i in range(groups - 1):
            value = value + theirs[which, i]
        return value

    beta = -dot_halves(inverse, halves(total(0)))
    beta_halves = halves(beta)
    swaps[1].wait()
    value = aside[...]
    for i in range(groups - 1):
        value = value + away[i]
    value = value + dot(proj_ref[...], beta_halves[0]) + dot(proj_ref[...], beta_halves[1])
    own = pl.ds(pl.multiple_of(me * rows, rows), rows)
    for t in range(groups):
        pl.when(col == t)(
            functools.partial(projs.__setitem__, (t, own), value[:, t * cols : (t + 1) * cols].astype(BF16))
        )
    gather = Gather(place, projs.at[col], rows, g_sends, g_recvs)
    gather.open()
    final_ref[...] = jnp.zeros_like(final_ref)

    def turn(i):
        at = pl.ds(i * chunk, chunk)
        right = beside([part_ref[t, at, :] for t in range(groups)])
        left = resid[at, :]
        pair = halves(left)
        sums[1] += dot_halves(pair, pair, TN)
        line = left + dot(right, beta_halves[0]) + dot(right, beta_halves[1])
        resid[at, :] = line
        pair = halves(line)
        final_ref[...] += dot_halves(pair, pair, TN)

    turns = [functools.partial(turn, i) for i in range(mine // chunk)]
    steps = gather.actions((m_sends, m_recvs, 0))
    cut = len(steps) * 2 // 3
    interleave(steps[:cut], turns)
    swaps.append(Swap(place, final_ref, shared, s_sends, s_recvs, 3 * groups, True))
    swaps.append(Swap(place, sums.at[1], theirs.at[1], s_sends, s_recvs, 2 * groups, True))
    feats = direction_ref.shape[0]
    owners = n // groups
    source = lax.div(me, owners)
    held = pl.ds(pl.multiple_of(lax.rem(me, owners) * feats, feats), feats)

    def copies():
        return [
            pltpu.make_async_remote_copy(
                src_ref=resid.at[held],
                dst_ref=resid.at[pl.ds(mine, feats)],
                send_sem=s_sends.at[4 * groups + i],
                recv_sem=s_recvs.at[4 * groups],
                device_id={"tgt": other},
                device_id_type=MESH,
            )
            for i, other in enumerate(place.others)
        ]

    @pl.when(col == source)
    def _():
        for copy in copies():
            copy.start()

    steps[cut]()
    swaps[0].drain()
    sums[0] = jnp.zeros((targets, targets), F32)

    def mix(s):
        block = beside([projs[t, gather.line(s), :] for t in range(groups)])
        sums[0] += dot(block, block, TN)

    mixed = 0
    for act in steps[cut + 1 :]:
        act()
        while mixed < min(place.lines, PLANE) - 2 and mixed in gather.mirrors:
            gather.mirrors[mixed].wait()
            mix(mixed)
            mixed += 1
    swaps[3].wait()
    new = total(1)
    for t in range(groups):
        pl.when(col == t)(functools.partial(target_ref.__setitem__, Ellipsis, new[:, t * cols : (t + 1) * cols]))
    for s in range(mixed, place.lines):
        gather.mirrors[s].wait()
    if place.lines - mixed <= PLANE:
        for s in range(mixed, place.lines):
            mix(s)
    else:
        def rest(s, carry):
            mix(s)
            return carry

        lax.fori_loop(mixed, place.lines, rest, 0)

    swaps[2].wait()
    swaps[2].drain()
    value = final_ref[...]
    for i in range(groups - 1):
        value = value + shared[i]
    final_ref[...] = ridge * value + sums[0] * (1.0 / total_n)

    @pl.when(col == source)
    def _():
        direction_ref[...] = resid[held, :]
        for copy in copies():
            copy.wait_send()

    @pl.when(col != source)
    def _():
        copies()[0].wait_recv()
        direction_ref[...] = resid[pl.ds(mine, feats), :]

    gather.drain()
    for swap in [swaps[1], swaps[3]]:
        swap.drain()


def second_stage(inverse, gram, lifted, part, proj, feats_own, feats):
    n, groups = lax.axis_size("samp"), lax.axis_size("tgt")
    _, mine, cols = lifted.shape
    rows = feats_own.shape[0]
    total_n, targets = rows * n, cols * groups
    return pl.pallas_call(
        functools.partial(second_kernel, n, groups, total_n),
        out_shape=[
            jax.ShapeDtypeStruct((targets, cols), F32),
            jax.ShapeDtypeStruct((targets, cols), F32),
            jax.ShapeDtypeStruct((targets, targets), F32),
            jax.ShapeDtypeStruct((feats, targets), F32),
        ],
        in_specs=[VMEM] * 6,
        out_specs=[VMEM] * 4,
        scratch_shapes=[
            pltpu.VMEM((mine + feats, targets), F32),
            pltpu.VMEM((2, targets, targets), F32),
            pltpu.VMEM((2, max(groups - 1, 1), targets, targets), F32),
            pltpu.VMEM((rows, targets), F32),
            pltpu.VMEM((max(groups - 1, 1), rows, targets), F32),
            pltpu.VMEM((groups, total_n, cols), BF16),
            pltpu.VMEM((max(groups - 1, 1), targets, targets), F32),
            pltpu.SemaphoreType.DMA((slots(n),)),
            pltpu.SemaphoreType.DMA((slots(n),)),
            pltpu.SemaphoreType.DMA((5 * groups,)),
            pltpu.SemaphoreType.DMA((5 * groups,)),
            pltpu.SemaphoreType.DMA((n // PLANE * groups,)),
            pltpu.SemaphoreType.DMA((n // PLANE * groups,)),
        ],
        compiler_params=pltpu.CompilerParams(collective_id=1, has_side_effects=True, vmem_limit_bytes=room(groups)),
        cost_estimate=pl.CostEstimate(flops=10**11, bytes_accessed=2 * 2**20, transcendentals=0),
        name="second",
    )(inverse, gram, lifted, part, proj, feats_own)


def body(samples, omega, phase, right_side):
    gram, mixed, lifted, part, proj, feats_own, right_all = first_stage(samples, omega, phase, right_side)
    inverse = inverse_of(mixed)
    first, target, final, direction = second_stage(
        inverse, gram, lifted, part, proj, feats_own, right_side.shape[0]
    )
    return last_solve(final, target, right_all, first, direction)


def solution(mesh):
    placed = (P("samp", None), P(), P(), P("samp", "tgt"))
    return jax.shard_map(
        body, mesh=mesh, in_specs=placed, out_specs=P("samp", "tgt"), check_vma=False
    )
```

```python
import functools

import jax
import jax.numpy as jnp
from jax import lax
from jax.experimental import pallas as pl
from jax.experimental.pallas import tpu as pltpu
from jax.sharding import PartitionSpec as P

ridge = 1.0
HI = lax.Precision.HIGHEST
F32 = jnp.float32
BF16 = jnp.bfloat16
BLOCK = 128
GROUP = 8
PLANE = 4
MESH = pl.DeviceIdType.MESH
NN = (((1,), (0,)), ((), ()))
TN = (((0,), (0,)), ((), ()))
NT = (((1,), (1,)), ((), ()))
VMEM = pl.BlockSpec(memory_space=pltpu.VMEM)


def precise_dot(left_matrix, right_matrix):
    return jnp.dot(left_matrix, right_matrix, precision=HI, preferred_element_type=F32)


def dot(left, right, dims=NN):
    return lax.dot_general(left, right, dims, preferred_element_type=F32)


def halves(x):
    high = x.astype(BF16)
    return high, (x - high.astype(F32)).astype(BF16)


def dot_halves(left, right, dims=NN):
    return dot(left[0], right[0], dims) + (dot(left[0], right[1], dims) + dot(left[1], right[0], dims))


def cosine(x):
    turns = x * 0.15915494309189535
    f = turns - jnp.round(turns)
    s = f * f
    p = -21.071105627575776
    for coef in (
        58.790492120100176,
        -85.27162153429538,
        64.92865742103322,
        -19.738980355764014,
        0.999999210782322,
    ):
        p = p * s + coef
    return p


def sweep(held):
    size = len(held)
    at = lambda i, j: held[max(i, j)][min(i, j)]
    for p in range(0, size, 2):
        q = p + 1
        a, b, c = held[p][p], held[q][p], held[q][q]
        scale = 1.0 / (a * c - b * b)
        pp, pq, qq = c * scale, b * scale, a * scale
        first, second = [at(i, p) for i in range(size)], [at(i, q) for i in range(size)]
        rest = [i for i in range(size) if i not in (p, q)]
        left = {i: first[i] * pp - second[i] * pq for i in rest}
        right = {i: second[i] * qq - first[i] * pq for i in rest}
        for i in rest:
            for j in rest:
                if j <= i:
                    held[i][j] = held[i][j] - (left[i] * first[j] + right[i] * second[j])
        for i in rest:
            held[max(i, p)][min(i, p)] = left[i]
            held[max(i, q)][min(i, q)] = right[i]
        held[p][p], held[q][p], held[q][q] = -pp, pq, -qq
    return [[-at(i, j) for j in range(size)] for i in range(size)]


def invert_block(value, unit):
    size = value.shape[0]
    tiles = [value[t * 8 : t * 8 + 8, :] for t in range(size // 8)]
    lane = lax.broadcasted_iota(jnp.int32, (8, size), 1)
    sub = lax.broadcasted_iota(jnp.int32, (8, size), 0)
    for g in range(size // GROUP):
        j = g * GROUP
        in_group = (lane >= j) & (lane < j + GROUP)
        home = tiles[g]
        spread = [jnp.broadcast_to(home[:, j + m : j + m + 1], (8, size)) * unit for m in range(GROUP)]
        rows = [
            jnp.where(in_group, jnp.where(lane == j + k, 1.0, 0.0), jnp.broadcast_to(home[k : k + 1, :], (8, size)))
            for k in range(GROUP)
        ]
        pivots = sweep(
            [[jnp.broadcast_to(spread[m][k : k + 1, :], (8, size)) for m in range(k + 1)] for k in range(GROUP)]
        )
        scaled = []
        for k in range(GROUP):
            terms = [pivots[k][m] * rows[m] for m in range(GROUP)]
            while len(terms) > 1:
                terms = [terms[i] + terms[i + 1] for i in range(0, len(terms), 2)]
            scaled.append(terms[0])
        nxt = []
        for t, tile in enumerate(tiles):
            if t == g:
                new = scaled[0]
                for k in range(1, GROUP):
                    new = jnp.where(sub == k, scaled[k], new)
            else:
                terms = [jnp.broadcast_to(tile[:, j + k : j + k + 1], (8, size)) * scaled[k] for k in range(GROUP)]
                while len(terms) > 1:
                    terms = [terms[i] + terms[i + 1] for i in range(0, len(terms), 2)]
                new = jnp.where(in_group, 0.0, tile) - terms[0]
            nxt.append(new)
        tiles = nxt
    return jnp.concatenate(tiles, axis=0)


def inverse_kernel(gram_ref, work, row, column, ones):
    total = gram_ref.shape[0]
    size = BLOCK
    count = total // size
    scale = 1.0 / jnp.max(gram_ref[...])
    work[...] = gram_ref[...] * scale
    row[...] = jnp.zeros_like(row)
    column[...] = jnp.zeros_like(column)
    ones[...] = jnp.ones_like(ones)

    def step(k, carry):
        at = pl.ds(pl.multiple_of(k * size, size), size)
        inv = invert_block(work[at, at], ones[...])
        for i in range(1, count):
            rows = pl.ds(pl.multiple_of(lax.rem(k + i, count) * size, size), size)
            work[rows, :] = work[rows, :] - precise_dot(column[rows, :], row[...])
        new = precise_dot(inv, work[at, :])
        for i in range(1, count):
            rows = pl.ds(pl.multiple_of(lax.rem(k + i, count) * size, size), size)
            column[rows, :] = work[rows, at]
            work[rows, at] = jnp.zeros((size, size), F32)
        work[at, :] = new
        work[at, at] = inv
        row[...] = new
        row[:, at] = inv
        soon = pl.ds(pl.multiple_of(lax.rem(k + 1, count) * size, size), size)
        work[soon, :] = work[soon, :] - precise_dot(column[soon, :], row[...])
        column[soon, :] = jnp.zeros((size, size), F32)
        column[at, :] = jnp.zeros((size, size), F32)
        return carry

    lax.fori_loop(0, count, step, 0)
    for i in range(count):
        rows = pl.ds(i * size, size)
        work[rows, :] = (work[rows, :] - precise_dot(column[rows, :], row[...])) * scale


def inverse_of(gram):
    total = gram.shape[0]
    return pl.pallas_call(
        inverse_kernel,
        out_shape=jax.ShapeDtypeStruct((total, total), F32),
        in_specs=[VMEM],
        out_specs=VMEM,
        scratch_shapes=[
            pltpu.VMEM((BLOCK, total), F32),
            pltpu.VMEM((total, BLOCK), F32),
            pltpu.VMEM((8, BLOCK), F32),
        ],
        compiler_params=pltpu.CompilerParams(vmem_limit_bytes=16 * 2**20),
        cost_estimate=pl.CostEstimate(flops=2 * 10**10, bytes_accessed=2 * 2**20, transcendentals=0),
        name="inverse",
    )(gram)


def last_kernel(gram_ref, rhs_ref, right_ref, first_ref, direction_ref, out_ref, work, row, column, ones):
    total, cols = rhs_ref.shape
    size = BLOCK
    count = total // size
    scale = 1.0 / jnp.max(gram_ref[...])
    work[:, :total] = gram_ref[...] * scale
    work[:, total:] = rhs_ref[...] * scale
    row[...] = jnp.zeros_like(row)
    column[...] = jnp.zeros_like(column)
    ones[...] = jnp.ones_like(ones)
    out_ref[...] = dot_halves(halves(right_ref[...]), halves(first_ref[...]))

    def step(k, carry):
        at = pl.ds(pl.multiple_of(k * size, size), size)
        inv = invert_block(work[at, at], ones[...])
        for i in range(1, count):
            rows = pl.ds(pl.multiple_of(lax.rem(k + i, count) * size, size), size)
            work[rows, :] = work[rows, :] - precise_dot(column[rows, :], row[...])
        new = precise_dot(inv, work[at, :])
        for i in range(1, count):
            rows = pl.ds(pl.multiple_of(lax.rem(k + i, count) * size, size), size)
            column[rows, :] = work[rows, at]
        work[at, :] = new
        row[...] = new
        soon = pl.ds(pl.multiple_of(lax.rem(k + 1, count) * size, size), size)
        work[soon, :] = work[soon, :] - precise_dot(column[soon, :], row[...])
        column[soon, :] = jnp.zeros((size, size), F32)
        column[at, :] = jnp.zeros((size, size), F32)
        return carry

    lax.fori_loop(0, count, step, 0)
    for i in range(count):
        rows = pl.ds(i * size, size)
        work[rows, total:] = work[rows, total:] - precise_dot(column[rows, :], row[:, total:])
    out_ref[...] += dot_halves(halves(direction_ref[...]), halves(work[:, total:]))


def last_solve(gram, rhs, right_all, first, direction):
    total, cols = rhs.shape
    return pl.pallas_call(
        last_kernel,
        out_shape=jax.ShapeDtypeStruct((direction.shape[0], cols), F32),
        in_specs=[VMEM] * 5,
        out_specs=VMEM,
        scratch_shapes=[
            pltpu.VMEM((total, total + cols), F32),
            pltpu.VMEM((BLOCK, total + cols), F32),
            pltpu.VMEM((total, BLOCK), F32),
            pltpu.VMEM((8, BLOCK), F32),
        ],
        compiler_params=pltpu.CompilerParams(vmem_limit_bytes=24 * 2**20),
        cost_estimate=pl.CostEstimate(flops=2 * 10**10, bytes_accessed=3 * 2**20, transcendentals=0),
        name="last",
    )(gram, rhs, right_all, first, direction)


class Place:
    def __init__(self, n, groups):
        self.n, self.groups, self.lines = n, groups, n // PLANE
        self.me, self.col = lax.axis_index("samp"), lax.axis_index("tgt")
        self.inner = lax.rem(self.me, PLANE)
        self.line = lax.div(self.me, PLANE)
        self.over_x = self.me + 1 - 2 * lax.rem(self.me, 2)
        self.over_y = self.me + 2 - 4 * lax.div(self.inner, 2)
        self.inner_x = lax.rem(self.over_x, PLANE)
        self.inner_y = lax.rem(self.over_y, PLANE)
        self.along = [lax.rem(self.line + s, self.lines) * PLANE + self.inner for s in range(1, self.lines)]
        self.others = [lax.rem(self.col + s, groups) for s in range(1, groups)]

    def greet(self):
        barrier = pltpu.get_barrier_semaphore()
        for peer in [*self.along, self.over_x, self.over_y]:
            pl.semaphore_signal(barrier, inc=1, device_id={"samp": peer}, device_id_type=MESH)
        for other in self.others:
            pl.semaphore_signal(barrier, inc=1, device_id={"tgt": other}, device_id_type=MESH)

    def meet(self):
        pl.semaphore_wait(pltpu.get_barrier_semaphore(), len(self.along) + 2 + len(self.others))

    def behind(self, s, inner):
        return lax.rem(self.line + self.lines - s, self.lines) * PLANE + inner


class Gather:
    def __init__(self, place, slab, rows, sends, recvs):
        self.place, self.slab, self.rows, self.sends, self.recvs = place, slab, rows, sends, recvs
        self.started, self.mirrors = [], {}
        self.z, self.x, self.y, self.d = {}, {}, {}, {}

    def span(self, block, part=None):
        if part is None:
            return self.slab.at[pl.ds(pl.multiple_of(block * self.rows, self.rows), self.rows)]
        half = self.rows // 2
        return self.slab.at[pl.ds(pl.multiple_of(block * self.rows + part * half, half), half)]

    def send(self, ref, slot, peer):
        copy = pltpu.make_async_remote_copy(
            src_ref=ref,
            dst_ref=ref,
            send_sem=self.sends.at[slot],
            recv_sem=self.recvs.at[slot],
            device_id={"samp": peer},
            device_id_type=MESH,
        )
        copy.start()
        self.started.append(copy)
        return copy

    def across(self, s):
        p = self.place
        ref = self.span(p.behind(s, p.inner))
        base = p.lines + 4 * s
        self.x[s] = self.send(ref, base, p.over_x)
        self.y[s] = self.send(ref, base + 1, p.over_y)

    def along(self):
        p = self.place
        for s in range(1, p.lines):
            self.z[s] = self.send(self.span(p.me), s, p.along[s - 1])

    def open(self):
        self.along()
        self.across(0)

    def relay(self, s):
        self.z[s].wait_recv()
        self.across(s)

    def corner(self, s):
        p = self.place
        base = p.lines + 4 * s
        self.x[s].wait_recv()
        one = self.send(self.span(p.behind(s, p.inner_x), 0), base + 2, p.over_y)
        self.y[s].wait_recv()
        self.d[s] = [one, self.send(self.span(p.behind(s, p.inner_y), 1), base + 3, p.over_x)]

    def line(self, s):
        size = PLANE * self.rows
        first = lax.rem(self.place.line + self.place.lines - s, self.place.lines)
        return pl.ds(pl.multiple_of(first * size, size), size)

    def finish(self, s, mirror=None):
        for copy in self.d[s]:
            copy.wait_recv()
        if mirror is not None:
            sends, recvs, base = mirror
            ref = self.slab.at[self.line(s)]
            self.mirrors[s] = Swap(self.place, ref, ref, sends, recvs, base + s * self.place.groups)

    def actions(self, mirror=None):
        lines = self.place.lines
        steps = [functools.partial(self.corner, 0)]
        steps += [functools.partial(self.relay, s) for s in range(1, min(lines, 4))]
        for s in range(1, lines):
            steps.append(functools.partial(self.corner, s))
            if s + 3 < lines:
                steps.append(functools.partial(self.relay, s + 3))
            if mirror is not None:
                steps.append(functools.partial(self.finish, s - 1, mirror))
        if mirror is not None:
            steps.append(functools.partial(self.finish, lines - 1, mirror))
        return steps

    def close(self):
        for s in range(self.place.lines):
            self.finish(s)

    def drain(self):
        for copy in self.started:
            copy.wait_send()
        for swap in self.mirrors.values():
            swap.drain()


def room(groups):
    return (63 if groups > 2 else 40) * 2**20


def slots(n):
    return n // PLANE + 4 * (n // PLANE)


class Swap:
    def __init__(self, place, src, dst, sends, recvs, base, slotted=False):
        self.copies = []
        for i, other in enumerate(place.others):
            copy = pltpu.make_async_remote_copy(
                src_ref=src,
                dst_ref=dst.at[i] if slotted else dst,
                send_sem=sends.at[base + i],
                recv_sem=recvs.at[base + i],
                device_id={"tgt": other},
                device_id_type=MESH,
            )
            copy.start()
            self.copies.append(copy)

    def wait(self):
        for copy in self.copies:
            copy.wait_recv()

    def drain(self):
        for copy in self.copies:
            copy.wait_send()


def interleave(actions, work, lead=0):
    done = min(lead, len(actions))
    for act in actions[:done]:
        act()
    rest = len(actions) - done
    for i, piece in enumerate(work):
        upto = len(actions) - rest + (i + 1) * rest // len(work)
        piece()
        for act in actions[done:upto]:
            act()
        done = upto


def beside(parts):
    return parts[0] if len(parts) == 1 else jnp.concatenate(parts, axis=1)


def first_kernel(
    n, groups, total_n,
    samples_hbm, omega_hbm, phase_hbm, right_hbm,
    gram_ref, mixed_ref, lifted_ref, part_ref, proj_ref, feats_ref, wide_ref,
    samples_ref, omega_ref, phase_ref, wides, spots, flat, rights, projs, lifts,
    loads, g_sends, g_recvs, s_sends, s_recvs, m_sends, m_recvs,
):
    place = Place(n, groups)
    me, col = place.me, place.col
    rows, depth = samples_ref.shape
    feats, cols = wides.shape[1:]
    total_f = omega_ref.shape[1]
    mine = total_f // groups
    pieces, piece = spots.shape[0], spots.shape[1] // n
    slab = col if pieces > 1 else 0

    fetches = [
        pltpu.make_async_copy(src, dst, loads.at[i])
        for i, (src, dst) in enumerate(
            [(samples_hbm, samples_ref), (right_hbm, wides.at[col]), (omega_hbm, omega_ref), (phase_hbm, phase_ref)]
        )
    ]
    for fetch in fetches:
        fetch.start()
    place.greet()
    fetches[0].wait()
    spots[slab, pl.ds(pl.multiple_of(me * piece, piece), piece), :] = samples_ref[
        pl.ds(pl.multiple_of(slab * piece, piece), piece), :
    ]
    fetches[1].wait()
    rights[col, pl.ds(pl.multiple_of(me * feats, feats), feats), :] = wides[col].astype(BF16)
    fetches[2].wait()
    fetches[3].wait()

    tile = 256

    def own_features(i, carry):
        at = pl.ds(pl.multiple_of(i * tile, tile), tile)
        feats_ref[:, at] = cosine(dot(samples_ref[...], omega_ref[:, at]) + phase_ref[:, at]).astype(BF16)
        return carry

    lax.fori_loop(0, total_f // tile, own_features, 0)
    place.meet()
    near = Gather(place, spots.at[slab], piece, g_sends.at[0], g_recvs.at[0])
    far = Gather(place, rights.at[col], feats, g_sends.at[1], g_recvs.at[1])
    near.open()
    far.open()
    swaps = [Swap(place, wides.at[col], wides.at[col], s_sends, s_recvs, 0)]
    for act in near.actions():
        act()
    near.close()
    if pieces > 1:
        swaps.append(Swap(place, spots.at[col], spots.at[col], s_sends, s_recvs, groups))
        swaps[-1].wait()

    def settle(b, carry):
        for t in range(pieces):
            flat[pl.ds(pl.multiple_of(b * rows + t * piece, piece), piece), :] = spots[
                t, pl.ds(pl.multiple_of(b * piece, piece), piece), :
            ]
        return carry

    lax.fori_loop(0, n, settle, 0)

    tiles = total_n // tile
    batch = 3 if tiles % 3 == 0 else 1

    def lift_features(c):
        at = pl.ds(pl.multiple_of(col * mine + c * tile, tile), tile)
        weights = omega_ref[:, at].T
        shift = jnp.broadcast_to(phase_ref[:, at], (128, tile)).T
        shift = jnp.concatenate([shift] * (tile // 128), axis=1)
        down = pl.ds(c * tile, tile)

        def one(i, carry):
            for b in range(batch):
                over = pl.ds(pl.multiple_of((i * batch + b) * tile, tile), tile)
                lifts[down, over] = cosine(dot(weights, flat[over, :], NT) + shift).astype(BF16)
            return carry

        lax.fori_loop(0, tiles // batch, one, 0)

    work = [functools.partial(lift_features, c) for c in range(mine // tile)]
    early = len(work) * 5 // 8
    interleave(far.actions(), work[:early], 3)
    far.close()
    spread = Swap(place, rights.at[col], rights.at[col], s_sends, s_recvs, 2 * groups)
    swaps.append(spread)
    projs[col, pl.ds(pl.multiple_of(me * rows, rows), rows), :] = dot(feats_ref[...], rights[col]).astype(BF16)
    last = Gather(place, projs.at[col], rows, g_sends.at[2], g_recvs.at[2])
    last.open()

    chunk = 512

    def gram_piece(lo, hi):
        def one(i, carry):
            at = pl.ds(pl.multiple_of(i * chunk, chunk), chunk)
            block = beside([rights[t, at, :] for t in range(groups)])
            gram_ref[...] += dot(block, block, TN)
            return carry

        lax.fori_loop(lo, hi, one, 0)

    gram_ref[...] = jnp.zeros_like(gram_ref)
    count = total_f // chunk
    steps = last.actions((m_sends, m_recvs, 0))
    ready = min(place.lines, PLANE) - 1
    mixed_ref[...] = jnp.zeros_like(mixed_ref)

    def absorb(s):
        block = beside([projs[t, last.line(s), :] for t in range(groups)])
        mixed_ref[...] += dot(block, block, TN)

    def lift(s, fresh):
        def one(i, carry):
            at = pl.ds(pl.multiple_of(i * chunk, chunk), chunk)
            left = lifts[at, last.line(s)]
            for t in range(groups):
                value = dot(left, projs[t, last.line(s), :]) * (1.0 / total_n)
                lifted_ref[t, at, :] = value if fresh else lifted_ref[t, at, :] + value
            return carry

        lax.fori_loop(0, mine // chunk, one, 0)

    grams = [functools.partial(gram_piece, i * count // 4, (i + 1) * count // 4) for i in range(4)]
    interleave(steps[:-2], [*work[early : early + 1], spread.wait, *grams, *work[early + 1 :]])
    used = 0
    for act in [*steps[-2:], lambda: None]:
        if used < ready and used in last.mirrors:
            last.mirrors[used].wait()
            absorb(used)
            lift(used, used == 0)
            used += 1
        act()
    for s in range(used, place.lines):
        last.mirrors[s].wait()
    if place.lines - used <= PLANE:
        for s in range(used, place.lines):
            absorb(s)
            lift(s, s == 0)
    else:
        def rest(s, carry):
            absorb(s)
            lift(s, False)
            return carry

        lax.fori_loop(used, place.lines, rest, 0)
    mixed_ref[...] = mixed_ref[...] * (1.0 / total_n) + ridge * gram_ref[...]

    own = pl.ds(pl.multiple_of(me * rows, rows), rows)
    swaps[0].wait()
    for t in range(groups):
        part_ref[t] = rights[t, pl.ds(pl.multiple_of(col * mine, mine), mine), :]
        proj_ref[:, t * cols : (t + 1) * cols] = projs[t, own, :]
        wide_ref[:, t * cols : (t + 1) * cols] = wides[t]
    for gather in (near, far, last):
        gather.drain()
    for swap in swaps:
        swap.drain()


def first_stage(samples, omega, phase, right_side):
    n, groups = lax.axis_size("samp"), lax.axis_size("tgt")
    rows, depth = samples.shape
    feats, cols = right_side.shape
    total_f = omega.shape[1]
    total_n, mine, targets = rows * n, total_f // groups, cols * groups
    pieces = groups if rows % (32 * groups) == 0 else 1
    return pl.pallas_call(
        functools.partial(first_kernel, n, groups, total_n),
        out_shape=[
            jax.ShapeDtypeStruct((targets, targets), F32),
            jax.ShapeDtypeStruct((targets, targets), F32),
            jax.ShapeDtypeStruct((groups, mine, cols), F32),
            jax.ShapeDtypeStruct((groups, mine, cols), BF16),
            jax.ShapeDtypeStruct((rows, targets), BF16),
            jax.ShapeDtypeStruct((rows, total_f), BF16),
            jax.ShapeDtypeStruct((feats, targets), F32),
        ],
        in_specs=[pl.BlockSpec(memory_space=pltpu.HBM)] * 4,
        out_specs=[VMEM] * 7,
        scratch_shapes=[
            pltpu.VMEM((rows, depth), BF16),
            pltpu.VMEM((depth, total_f), BF16),
            pltpu.VMEM((1, total_f), F32),
            pltpu.VMEM((groups, feats, cols), F32),
            pltpu.VMEM((pieces, total_n // pieces, depth), BF16),
            pltpu.VMEM((total_n, depth), BF16),
            pltpu.VMEM((groups, total_f, cols), BF16),
            pltpu.VMEM((groups, total_n, cols), BF16),
            pltpu.VMEM((mine, total_n), BF16),
            pltpu.SemaphoreType.DMA((4,)),
            pltpu.SemaphoreType.DMA((3, slots(n))),
            pltpu.SemaphoreType.DMA((3, slots(n))),
            pltpu.SemaphoreType.DMA((3 * groups,)),
            pltpu.SemaphoreType.DMA((3 * groups,)),
            pltpu.SemaphoreType.DMA((n // PLANE * groups,)),
            pltpu.SemaphoreType.DMA((n // PLANE * groups,)),
        ],
        compiler_params=pltpu.CompilerParams(collective_id=0, has_side_effects=True, vmem_limit_bytes=room(groups)),
        cost_estimate=pl.CostEstimate(flops=10**11, bytes_accessed=2 * 2**20, transcendentals=0),
        name="first",
    )(*[pltpu.with_memory_space_constraint(x, pltpu.HBM) for x in (samples, omega, phase.reshape(1, -1), right_side)])


def second_kernel(
    n, groups, total_n,
    inverse_ref, gram_ref, lifted_ref, part_ref, proj_ref, feats_ref,
    first_ref, target_ref, final_ref, direction_ref,
    resid, sums, theirs, aside, away, projs, shared, g_sends, g_recvs, s_sends, s_recvs, m_sends, m_recvs,
):
    place = Place(n, groups)
    me, col = place.me, place.col
    rows = feats_ref.shape[0]
    mine, cols = lifted_ref.shape[1:]
    targets = groups * cols
    chunk = 512
    place.greet()
    inverse = halves(inverse_ref[...])
    alpha = dot_halves(inverse, halves(gram_ref[...]))
    alpha_halves = halves(alpha)
    for t in range(groups):
        pl.when(col == t)(functools.partial(first_ref.__setitem__, Ellipsis, alpha[:, t * cols : (t + 1) * cols]))
    sums[...] = jnp.zeros_like(sums)
    aside[...] = jnp.zeros_like(aside)

    def one(i, carry):
        at = pl.ds(pl.multiple_of(i * chunk, chunk), chunk)
        right = beside([part_ref[t, at, :] for t in range(groups)]).astype(F32)
        image = halves(beside([lifted_ref[t, at, :] for t in range(groups)]) + ridge * right)
        left = right - dot_halves(image, alpha_halves)
        resid[at, :] = left
        pair = halves(left)
        sums[0] += dot_halves(image, pair, TN)
        over = pl.ds(pl.multiple_of(col * mine + i * chunk, chunk), chunk)
        aside[...] += dot(feats_ref[:, over], pair[0])
        return carry

    lax.fori_loop(0, mine // chunk, one, 0)
    place.meet()
    swaps = [
        Swap(place, sums.at[0], theirs.at[0], s_sends, s_recvs, 0, True),
        Swap(place, aside, away, s_sends, s_recvs, groups, True),
    ]
    swaps[0].wait()

    def total(which):
        value = sums[which]
        for i in range(groups - 1):
            value = value + theirs[which, i]
        return value

    beta = -dot_halves(inverse, halves(total(0)))
    beta_halves = halves(beta)
    swaps[1].wait()
    value = aside[...]
    for i in range(groups - 1):
        value = value + away[i]
    value = value + dot(proj_ref[...], beta_halves[0]) + dot(proj_ref[...], beta_halves[1])
    own = pl.ds(pl.multiple_of(me * rows, rows), rows)
    for t in range(groups):
        pl.when(col == t)(
            functools.partial(projs.__setitem__, (t, own), value[:, t * cols : (t + 1) * cols].astype(BF16))
        )
    gather = Gather(place, projs.at[col], rows, g_sends, g_recvs)
    gather.open()
    final_ref[...] = jnp.zeros_like(final_ref)

    def turn(i):
        at = pl.ds(i * chunk, chunk)
        right = beside([part_ref[t, at, :] for t in range(groups)])
        left = resid[at, :]
        pair = halves(left)
        sums[1] += dot_halves(pair, pair, TN)
        line = left + dot(right, beta_halves[0]) + dot(right, beta_halves[1])
        resid[at, :] = line
        pair = halves(line)
        final_ref[...] += dot_halves(pair, pair, TN)

    turns = [functools.partial(turn, i) for i in range(mine // chunk)]
    steps = gather.actions((m_sends, m_recvs, 0))
    cut = len(steps) * 2 // 3
    interleave(steps[:cut], turns)
    swaps.append(Swap(place, final_ref, shared, s_sends, s_recvs, 3 * groups, True))
    swaps.append(Swap(place, sums.at[1], theirs.at[1], s_sends, s_recvs, 2 * groups, True))
    feats = direction_ref.shape[0]
    owners = n // groups
    source = lax.div(me, owners)
    held = pl.ds(pl.multiple_of(lax.rem(me, owners) * feats, feats), feats)

    def copies():
        return [
            pltpu.make_async_remote_copy(
                src_ref=resid.at[held],
                dst_ref=resid.at[pl.ds(mine, feats)],
                send_sem=s_sends.at[4 * groups + i],
                recv_sem=s_recvs.at[4 * groups],
                device_id={"tgt": other},
                device_id_type=MESH,
            )
            for i, other in enumerate(place.others)
        ]

    @pl.when(col == source)
    def _():
        for copy in copies():
            copy.start()

    steps[cut]()
    swaps[0].drain()
    sums[0] = jnp.zeros((targets, targets), F32)

    def mix(s):
        block = beside([projs[t, gather.line(s), :] for t in range(groups)])
        sums[0] += dot(block, block, TN)

    mixed = 0
    for act in steps[cut + 1 :]:
        act()
        while mixed < min(place.lines, PLANE) - 2 and mixed in gather.mirrors:
            gather.mirrors[mixed].wait()
            mix(mixed)
            mixed += 1
    swaps[3].wait()
    new = total(1)
    for t in range(groups):
        pl.when(col == t)(functools.partial(target_ref.__setitem__, Ellipsis, new[:, t * cols : (t + 1) * cols]))
    for s in range(mixed, place.lines):
        gather.mirrors[s].wait()
    if place.lines - mixed <= PLANE:
        for s in range(mixed, place.lines):
            mix(s)
    else:
        def rest(s, carry):
            mix(s)
            return carry

        lax.fori_loop(mixed, place.lines, rest, 0)

    swaps[2].wait()
    swaps[2].drain()
    value = final_ref[...]
    for i in range(groups - 1):
        value = value + shared[i]
    final_ref[...] = ridge * value + sums[0] * (1.0 / total_n)

    @pl.when(col == source)
    def _():
        direction_ref[...] = resid[held, :]
        for copy in copies():
            copy.wait_send()

    @pl.when(col != source)
    def _():
        copies()[0].wait_recv()
        direction_ref[...] = resid[pl.ds(mine, feats), :]

    gather.drain()
    for swap in [swaps[1], swaps[3]]:
        swap.drain()


def second_stage(inverse, gram, lifted, part, proj, feats_own, feats):
    n, groups = lax.axis_size("samp"), lax.axis_size("tgt")
    _, mine, cols = lifted.shape
    rows = feats_own.shape[0]
    total_n, targets = rows * n, cols * groups
    return pl.pallas_call(
        functools.partial(second_kernel, n, groups, total_n),
        out_shape=[
            jax.ShapeDtypeStruct((targets, cols), F32),
            jax.ShapeDtypeStruct((targets, cols), F32),
            jax.ShapeDtypeStruct((targets, targets), F32),
            jax.ShapeDtypeStruct((feats, targets), F32),
        ],
        in_specs=[VMEM] * 6,
        out_specs=[VMEM] * 4,
        scratch_shapes=[
            pltpu.VMEM((mine + feats, targets), F32),
            pltpu.VMEM((2, targets, targets), F32),
            pltpu.VMEM((2, max(groups - 1, 1), targets, targets), F32),
            pltpu.VMEM((rows, targets), F32),
            pltpu.VMEM((max(groups - 1, 1), rows, targets), F32),
            pltpu.VMEM((groups, total_n, cols), BF16),
            pltpu.VMEM((max(groups - 1, 1), targets, targets), F32),
            pltpu.SemaphoreType.DMA((slots(n),)),
            pltpu.SemaphoreType.DMA((slots(n),)),
            pltpu.SemaphoreType.DMA((5 * groups,)),
            pltpu.SemaphoreType.DMA((5 * groups,)),
            pltpu.SemaphoreType.DMA((n // PLANE * groups,)),
            pltpu.SemaphoreType.DMA((n // PLANE * groups,)),
        ],
        compiler_params=pltpu.CompilerParams(collective_id=1, has_side_effects=True, vmem_limit_bytes=room(groups)),
        cost_estimate=pl.CostEstimate(flops=10**11, bytes_accessed=2 * 2**20, transcendentals=0),
        name="second",
    )(inverse, gram, lifted, part, proj, feats_own)


def body(samples, omega, phase, right_side):
    gram, mixed, lifted, part, proj, feats_own, right_all = first_stage(samples, omega, phase, right_side)
    inverse = inverse_of(mixed)
    first, target, final, direction = second_stage(
        inverse, gram, lifted, part, proj, feats_own, right_side.shape[0]
    )
    return last_solve(final, target, right_all, first, direction)


def solution(mesh):
    placed = (P("samp", None), P(), P(), P("samp", "tgt"))
    return jax.shard_map(
        body, mesh=mesh, in_specs=placed, out_specs=P("samp", "tgt"), check_vma=False
    )
```
